32 devices in a mesh: dp: 4 (over y, x), expert: 8 (over z, core).
Axes of the slice: x: 2, y: 2, z: 4, core: 2. Of those that a mesh axis runs over, the one named last changes fastest.
Arguments:
- tokens: bfloat16 [16384, 2048], P(('dp', 'expert')), may hold values from -6 to 6
- expert_ids: int32 [16384, 1], P(('dp', 'expert')), may hold values from 0 to 7; in each aligned block of 512 rows (0 to 511, 512 to 1023, ...) at most 128 rows name the same one
- gate_proj: bfloat16 [8, 2048, 768], P('expert'), may hold values from -0.125 to 0.125
- up_proj: bfloat16 [8, 2048, 768], P('expert'), may hold values from -0.125 to 0.125
- down_proj: bfloat16 [8, 768, 2048], P('expert'), may hold values from -0.21875 to 0.21875
Outputs:
- mixed: bfloat16 [16384, 2048], P(('dp', 'expert'))
- slot_index: int32 [16384], P(('dp', 'expert'))
The draws below stay inside these ranges and needn't reach their ends.
Inputs may be any that keep to these rules, and one draw needn't show every extreme that they name: `expert_ids`: among the rows of one device no expert is named more than 128 times; in some devices' rows one expert is named exactly 128 times.
All inputs are finite; a program needn't handle non-finite values.
Results may differ from the reference program's by a relative error of at most 0.0046.
The reference program's roundings to bfloat16 on the way (of `hidden`) count: a program that leaves them out, or rounds other values in their place, can miss the bound.
Values may be sent and summed in bfloat16 or wider, within the bound.
A program may use at most 64 MiB of HBM per device.

```python
import math
import jax
import jax.numpy as jnp
import numpy as np
from jax import lax

D = 2048
FF = 768
TOK_DEV = 512
EXPERTS = 8
TOKENS = 16384
MOST = 128
CAP = 2048


def block_scale(own_key, dims, pieces, least, high):
    loudness, own = 1.0, jax.random.fold_in(own_key, 6)
    for position, blocks in pieces:
        draws = jnp.exp(jax.random.uniform(jax.random.fold_in(own, position), (blocks,), jnp.float32, least / len(pieces), high / len(pieces)))
        loudness = loudness * jnp.repeat(draws, dims[position] // blocks).reshape([-1 if axis == position else 1 for axis in range(len(dims))])
    return loudness


def routed_block(stream_key, own, number, rows, number_of, top, reach, lean):
    sequence = jax.random.permutation(stream_key, number_of)
    crowded, common = portions_of(number_of, rows * top, reach, lean, True), portions_of(number_of, rows * top, reach, lean, False)
    places = jnp.arange(number_of)

    def named(sizes, turn):
        used = int((sizes > 0).sum())
        fixed = max(1, used // 4)
        shifted = fixed + (places - fixed + turn * (used - fixed)) % max(1, number_of - fixed)
        return jnp.zeros((number_of,), jnp.int32).at[sequence[jnp.where(places < fixed, places, shifted)]].set(jnp.asarray(sizes, jnp.int32))

    sizes = jnp.where(number % 4 == 0, named(crowded, number // 4), named(common, number - number // 4 - 1))
    mixed = jax.random.permutation(jax.random.fold_in(own, 3), number_of)
    donor, taker = mixed[0:number_of // 2 * 2:2], mixed[1:number_of // 2 * 2:2]
    slack = jnp.minimum(sizes[donor] - 1, reach - sizes[taker]) // 2
    slack = jnp.where((donor == sequence[0]) | (taker == sequence[0]) | (sizes[taker] == 0), 0, jnp.maximum(slack, 0))
    shifted = jax.random.randint(jax.random.fold_in(own, 4), (number_of // 2,), 0, 1 << 20) % (slack + 1)
    sizes = sizes.at[donor].add(-shifted).at[taker].add(shifted)
    items = jnp.searchsorted(jnp.cumsum(sizes), jnp.arange(rows * top), side="right").astype(jnp.int32)
    table = items.reshape(top, rows).T
    table = table[jax.random.permutation(jax.random.fold_in(own, 1), rows)]
    turn = jax.random.randint(jax.random.fold_in(own, 2), (rows, 1), 0, top)
    return jnp.take_along_axis(table, (jnp.arange(top)[None, :] + turn) % top, axis=1)


def portions_of(number_of, total, most, slope, full):
    weights = [(1 << 20) // math.isqrt(standing ** slope) + 1 for standing in range(1, number_of + 1)]
    largest = most if full else min(most, max(-(-total // number_of), total * weights[0] // sum(weights)))
    least = 1 if total - largest >= number_of - 1 else 0
    holding, rest = [largest] + [least] * (number_of - 1), total - largest - least * (number_of - 1)
    while rest > 0:
        candidates = [i for i in range(1, number_of) if holding[i] < largest] or [i for i in range(1, number_of) if holding[i] < most]
        pool, left = sum([weights[i] for i in candidates]), rest
        for i in candidates:
            more = min(most - holding[i], max(1, left * weights[i] // pool), rest)
            holding[i] = holding[i] + more
            rest = rest - more
    return np.array(holding)


def scatter_about(key, dims, spread, bound, cuts=(), kind=jnp.bfloat16):
    factor_of = block_scale(key, dims, cuts, -0.22, 0.18) if cuts else 1.0
    result = jax.random.normal(key, dims, jnp.float32) * spread * factor_of
    return jnp.minimum(jnp.maximum(result, -bound), bound).astype(kind)


def setup_inputs(seed: int = 0) -> dict:
    arg_keys = jax.random.split(jax.random.key(seed), 6)
    tokens = scatter_about(arg_keys[0], (TOKENS, D), 1.0, 6.0, ((0, 32),))
    expert_ids_keys = jax.random.split(jax.random.fold_in(arg_keys[1], 1), TOKENS // TOK_DEV)
    expert_ids_turns = jax.random.permutation(jax.random.fold_in(arg_keys[1], 3), TOKENS // TOK_DEV)
    expert_ids = jax.vmap(lambda own, number: routed_block(jax.random.fold_in(arg_keys[1], 2), own, number, TOK_DEV, EXPERTS, 1, MOST, 2))(expert_ids_keys, expert_ids_turns).reshape((TOKENS, 1))
    gate_proj = scatter_about(arg_keys[2], (EXPERTS, D, FF), D ** -0.5, 0.125, ((0, 8),))
    up_proj = scatter_about(arg_keys[3], (EXPERTS, D, FF), D ** -0.5, 0.125, ((0, 8),))
    down_proj = scatter_about(arg_keys[4], (EXPERTS, FF, D), FF ** -0.5, 0.21875, ((0, 8),))
    return {"tokens": tokens, "expert_ids": expert_ids, "gate_proj": gate_proj, "up_proj": up_proj, "down_proj": down_proj}


def expert_ffn(args):
    rows, gate_w, up_w, down_w = args
    gate_val = jnp.dot(rows, gate_w, preferred_element_type=jnp.float32)
    up_val = jnp.dot(rows, up_w, preferred_element_type=jnp.float32)
    hidden = (jax.nn.silu(gate_val) * up_val).astype(jnp.bfloat16)
    return jnp.dot(hidden, down_w, preferred_element_type=jnp.float32).astype(jnp.bfloat16)


def reference(tokens, expert_ids, gate_proj, up_proj, down_proj):
    choices = expert_ids[:, 0].astype(jnp.int32)
    onehot = (choices[:, None] == jnp.arange(EXPERTS, dtype=jnp.int32)[None, :]).astype(jnp.int32)
    before = jnp.cumsum(onehot, axis=0) - onehot
    slot_index = jnp.sum(before * onehot, axis=1).astype(jnp.int32)
    is_kept = slot_index < CAP
    buffer = jnp.zeros((EXPERTS, CAP, D), tokens.dtype)
    buffer = buffer.at[choices, slot_index].set(tokens, mode="drop")
    results = lax.map(expert_ffn, (buffer, gate_proj, up_proj, down_proj))
    picked = results[choices, jnp.minimum(slot_index, CAP - 1)]
    mixed = jnp.where(is_kept[:, None], picked, jnp.zeros_like(picked))
    return mixed, slot_index
```

```python
import functools

import jax
import jax.numpy as jnp
from jax import lax
from jax.experimental import pallas as pl
from jax.experimental.pallas import tpu as pltpu
from jax.sharding import PartitionSpec as P

MESH = pl.DeviceIdType.MESH
F32 = jnp.float32
BF16 = jnp.bfloat16
LANES = 128
NEAR_BLOCKS, FAR_BLOCKS, GO_BLOCKS, DELAY = 18, 19, 13, 3


def spread(step, n):
    half = (step // 2) * (2 * (step % 2) - 1)
    return jnp.where(step == 0, 0, n // 2 + half)


def direct_kernel(
    n, dps, most, capacity,
    row_ids, col_ids, tok_ref, gate_hbm, up_hbm, down_hbm,
    out_ref, slot_ref,
    gate_ref, up_ref, down_ref, outgoing, arrived, results, returned,
    position, offset, counts, count_all, totals, total_all,
    weight_sem, go_send, go_recv, back_send, back_recv,
    count_send, count_recv, total_send, total_recv,
):
    me = lax.axis_index("expert")
    group = lax.axis_index("dp")
    tok = tok_ref.shape[0]
    width = tok_ref.shape[1]

    weights = [
        pltpu.make_async_copy(src.at[0], dst, weight_sem.at[i])
        for i, (src, dst) in enumerate(
            ((gate_hbm, gate_ref), (up_hbm, up_ref), (down_hbm, down_ref))
        )
    ]
    for copy in weights:
        copy.start()

    barrier = pltpu.get_barrier_semaphore()

    def greet(i, c):
        pl.semaphore_signal(
            barrier, inc=1, device_id={"expert": lax.rem(me + i, n)}, device_id_type=MESH
        )
        return c

    def greet_dp(i, c):
        pl.semaphore_signal(
            barrier, inc=1, device_id={"dp": lax.rem(group + i, dps)}, device_id_type=MESH
        )
        return c

    lax.fori_loop(1, n, greet, 0)
    lax.fori_loop(1, dps, greet_dp, 0)

    earlier = lax.broadcasted_iota(jnp.int32, (tok, tok), 0) < lax.broadcasted_iota(
        jnp.int32, (tok, tok), 1
    )
    later = lax.broadcasted_iota(jnp.int32, (tok, tok), 0) > lax.broadcasted_iota(
        jnp.int32, (tok, tok), 1
    )
    ids_row = row_ids[...]
    hot_row = (ids_row == lax.broadcasted_iota(jnp.int32, (n, tok), 0)).astype(F32)
    before_row = jnp.dot(
        hot_row.astype(BF16), earlier.astype(F32).astype(BF16), preferred_element_type=F32
    )
    rank_row = jnp.sum(before_row * hot_row, axis=0, keepdims=True).astype(jnp.int32)
    pos_row = ids_row * most + rank_row
    counts[...] = jnp.broadcast_to(
        jnp.sum(hot_row, axis=1, keepdims=True), (n, LANES)
    ).astype(jnp.int32)

    ids_col = col_ids[...]
    hot_col = (ids_col == lax.broadcasted_iota(jnp.int32, (tok, n), 1)).astype(F32)
    before_col = jnp.dot(
        later.astype(F32).astype(BF16), hot_col.astype(BF16), preferred_element_type=F32
    )
    rank_col = jnp.sum(before_col * hot_col, axis=1, keepdims=True).astype(jnp.int32)
    position[...] = ids_col * most + rank_col

    def go(dest, source):
        return pltpu.make_async_remote_copy(
            src_ref=outgoing.at[dest], dst_ref=arrived.at[source],
            send_sem=go_send.at[dest], recv_sem=go_recv.at[source],
            device_id={"expert": dest}, device_id_type=MESH,
        )

    def back(dest, source):
        return pltpu.make_async_remote_copy(
            src_ref=results.at[dest], dst_ref=returned.at[source],
            send_sem=back_send.at[dest], recv_sem=back_recv.at[source],
            device_id={"expert": dest}, device_id_type=MESH,
        )

    def count(dest, source):
        return pltpu.make_async_remote_copy(
            src_ref=counts, dst_ref=count_all.at[source],
            send_sem=count_send.at[dest], recv_sem=count_recv.at[source],
            device_id={"expert": dest}, device_id_type=MESH,
        )

    def total(dest, source):
        return pltpu.make_async_remote_copy(
            src_ref=totals, dst_ref=total_all.at[source],
            send_sem=total_send.at[dest], recv_sem=total_recv.at[source],
            device_id={"dp": dest}, device_id_type=MESH,
        )

    def pack(dest):
        pick = (
            lax.broadcasted_iota(jnp.int32, (most, tok), 0) + dest * most == pos_row
        ).astype(F32).astype(BF16)
        return jnp.dot(pick, tok_ref[...], preferred_element_type=F32).astype(BF16)

    pl.semaphore_wait(barrier, n + dps - 2)

    def dispatch(i, c):
        dest = lax.rem(me + spread(i, n), n)
        outgoing[dest] = pack(dest)
        go(dest, me).start()
        return c

    lax.fori_loop(1, n, dispatch, 0)

    def tell(i, c):
        count(lax.rem(me + i, n), me).start()
        return c

    lax.fori_loop(1, n, tell, 0)
    count_all[me] = counts[...]
    arrived[me] = pack(me)

    for copy in weights:
        copy.wait()

    def ffn(source):
        rows = arrived[source]
        gate = jnp.dot(rows, gate_ref[...], preferred_element_type=F32)
        up = jnp.dot(rows, up_ref[...], preferred_element_type=F32)
        hidden = (gate / (1.0 + jnp.exp(-gate)) * up).astype(BF16)
        return jnp.dot(hidden, down_ref[...], preferred_element_type=F32).astype(BF16)

    def expert_step(i, c):
        source = lax.rem(me + n - spread(i, n), n)

        @pl.when(i > 0)
        def _():
            go(me, source).wait_recv()

        results[source] = ffn(source)

        @pl.when(i > 0)
        def _():
            back(source, me).start()

        return c

    lax.fori_loop(0, n, expert_step, 0)

    def heard(i, c):
        count(me, lax.rem(me + i, n)).wait_recv()
        return c

    lax.fori_loop(1, n, heard, 0)

    def add(i, carry):
        inner, whole = carry
        here = count_all[i]
        return inner + here * (i < me).astype(jnp.int32), whole + here

    zero = jnp.zeros((n, LANES), jnp.int32)
    inner, whole = lax.fori_loop(0, n, add, (zero, zero))
    totals[...] = whole

    def tell_dp(i, c):
        total(lax.rem(group + i, dps), group).start()
        return c

    lax.fori_loop(1, dps, tell_dp, 0)
    total_all[group] = whole

    def heard_dp(i, c):
        total(group, lax.rem(group + i, dps)).wait_recv()
        return c

    lax.fori_loop(1, dps, heard_dp, 0)

    def add_dp(i, outer):
        return outer + total_all[i] * (i < group).astype(jnp.int32)

    offset[...] = inner + lax.fori_loop(0, dps, add_dp, zero)
    slot_ref[...] = (
        jnp.sum(
            hot_row * offset[:, 0:1].astype(F32), axis=0, keepdims=True
        ).astype(jnp.int32)
        + rank_row
    )

    piece = min(width, 512)

    def combine(source, block, first):
        lane = lax.broadcasted_iota(jnp.int32, (tok, most), 1)
        fits = offset[pl.ds(source, 1), 0:most] + lax.broadcasted_iota(
            jnp.int32, (1, most), 1
        ) < capacity
        pick = (lane + source * most == position[...]) & fits
        pick = pick.astype(F32).astype(BF16)
        for at in range(0, width, piece):
            part = jnp.dot(
                pick, block[source, :, at : at + piece], preferred_element_type=F32
            ).astype(BF16)
            if first:
                out_ref[:, at : at + piece] = part
            else:
                out_ref[:, at : at + piece] += part

    combine(me, results, True)

    def combine_step(i, c):
        source = lax.rem(me + n - spread(i, n), n)
        back(me, source).wait_recv()
        combine(source, returned, False)
        return c

    lax.fori_loop(1, n, combine_step, 0)

    def drain(i, c):
        other = lax.rem(me + i, n)
        go(other, me).wait_send()
        back(other, me).wait_send()
        count(other, me).wait_send()
        return c

    lax.fori_loop(1, n, drain, 0)

    def drain_dp(i, c):
        total(lax.rem(group + i, dps), group).wait_send()
        return c

    lax.fori_loop(1, dps, drain_dp, 0)


def direct(tokens, expert_ids, gate_proj, up_proj, down_proj):
    tok, width = tokens.shape
    hidden = gate_proj.shape[2]
    n = lax.axis_size("expert")
    dps = lax.axis_size("dp")
    most = 2 * tok // n
    capacity = tok * dps
    vmem = pl.BlockSpec(memory_space=pltpu.VMEM)
    anywhere = pl.BlockSpec(memory_space=pltpu.MemorySpace.HBM)
    dma = pltpu.SemaphoreType.DMA
    block = pltpu.VMEM((n, most, width), BF16)
    mixed, slot = pl.pallas_call(
        functools.partial(direct_kernel, n, dps, most, capacity),
        out_shape=(
            jax.ShapeDtypeStruct((tok, width), BF16),
            jax.ShapeDtypeStruct((1, tok), jnp.int32),
        ),
        in_specs=[vmem, vmem, vmem, anywhere, anywhere, anywhere],
        out_specs=(vmem, vmem),
        scratch_shapes=[
            pltpu.VMEM((width, hidden), BF16),
            pltpu.VMEM((width, hidden), BF16),
            pltpu.VMEM((hidden, width), BF16),
            block, block, block, block,
            pltpu.VMEM((tok, 1), jnp.int32),
            pltpu.VMEM((n, LANES), jnp.int32),
            pltpu.VMEM((n, LANES), jnp.int32),
            pltpu.VMEM((n, n, LANES), jnp.int32),
            pltpu.VMEM((n, LANES), jnp.int32),
            pltpu.VMEM((dps, n, LANES), jnp.int32),
            dma((3,)), dma((n,)), dma((n,)), dma((n,)), dma((n,)),
            dma((n,)), dma((n,)), dma((dps,)), dma((dps,)),
        ],
        compiler_params=pltpu.CompilerParams(
            collective_id=0, has_side_effects=True, vmem_limit_bytes=60 * 2**20
        ),
    )(
        expert_ids.reshape(1, tok), expert_ids, tokens, gate_proj, up_proj, down_proj
    )
    return mixed, slot.reshape(tok)


def entering(part, axis, combine, identity):
    place = lax.axis_index(axis)
    gathered = lax.all_gather(part, axis)
    state = jnp.zeros_like(part) + jnp.asarray(identity, part.dtype)

    def one(hop, state):
        return combine(state, lax.dynamic_index_in_dim(gathered, hop, 0, False))

    return lax.fori_loop(0, place, one, state)


def add_counts(earlier, later):
    return earlier + later


def expert_ffn(rows, gate_proj, up_proj, down_proj):
    gate_val = jnp.dot(rows, gate_proj[0], preferred_element_type=jnp.float32)
    up_val = jnp.dot(rows, up_proj[0], preferred_element_type=jnp.float32)
    hidden = (jax.nn.silu(gate_val) * up_val).astype(jnp.bfloat16)
    return jnp.dot(hidden, down_proj[0], preferred_element_type=jnp.float32).astype(jnp.bfloat16)


def padded(tokens, expert_ids, gate_proj, up_proj, down_proj):
    tok_rows, width = tokens.shape
    experts_all = lax.axis_size("expert")
    most = 2 * tok_rows // experts_all
    capacity = tok_rows * lax.axis_size("dp")
    choices = expert_ids[:, 0]
    onehot = (choices[:, None] == jnp.arange(experts_all, dtype=jnp.int32)[None, :]).astype(
        jnp.int32
    )
    counts = jnp.sum(onehot, axis=0)
    inner = entering(counts, "expert", add_counts, jnp.zeros_like(counts))
    totals = lax.psum(counts, "expert")
    outer = entering(totals, "dp", add_counts, jnp.zeros_like(totals))
    offset = inner + outer
    before = jnp.cumsum(onehot, axis=0) - onehot
    local_rank = jnp.sum(before * onehot, axis=1)
    global_slot = (jnp.sum(onehot * offset[None, :], axis=1) + local_rank).astype(jnp.int32)
    is_kept = global_slot < capacity
    position = choices * most + local_rank
    targets = jnp.arange(experts_all * most, dtype=jnp.int32)
    dispatch = ((targets[:, None] == position[None, :]) & is_kept[None, :]).astype(jnp.bfloat16)
    outgoing = jnp.dot(dispatch, tokens, preferred_element_type=jnp.float32).astype(jnp.bfloat16)
    outgoing = outgoing.reshape(experts_all, most, width)
    arrived = lax.all_to_all(outgoing, "expert", split_axis=0, concat_axis=0, tiled=True)
    sources, slots_here, _ = arrived.shape
    flat = arrived.reshape(sources * slots_here, width)
    returned = lax.all_to_all(
        expert_ffn(flat, gate_proj, up_proj, down_proj).reshape(sources, slots_here, width),
        "expert",
        split_axis=0,
        concat_axis=0,
        tiled=True,
    )
    flat_back = returned.reshape(experts_all * most, width)
    mixed = lax.dot_general(
        dispatch, flat_back, (((0,), (0,)), ((), ())), preferred_element_type=jnp.float32
    )
    return (mixed.astype(jnp.bfloat16), global_slot)


NEAR_ORDER = {
    "A": (("go", "o", "p"), ("go", "o", "q"), ("go", "o", "i"),
          ("ret", "o", "i"), ("ret", "o", "p"), ("ret", "o", "q")),
    "M": (("go", "i", "p"), ("go", "i", "q"), ("go", "o", "p"), ("go", "o", "q"),
          ("ret", "i", "p"), ("ret", "i", "q"), ("ret", "o", "p"), ("ret", "o", "q")),
    "B": (("go", "i", "o"), ("go", "p", "o"), ("go", "q", "o"),
          ("ret", "i", "o"), ("ret", "p", "o"), ("ret", "q", "o")),
}
FLIP = {"o": "q", "i": "p", "p": "i", "q": "o"}
FAR_KEY = 4096
LOCAL_KEY = 8192


def lay_streams(rows_of, block, delay):
    place, end = {}, {}
    queue = {(s, h): list(NEAR_ORDER[s]) for s in "AMB" for h in (0, 1)}
    zero = jnp.zeros((1, LANES), jnp.int32)
    for name in queue:
        end[name] = zero
    while any(queue.values()):
        for (s, h), runs in queue.items():
            while runs:
                kind, a, b = runs[0]
                fa, fb = FLIP[a], FLIP[b]
                need = None
                if s == "A" and kind == "ret":
                    need = (("B", h, "go", b, a), 3 + delay)
                elif s == "M" and a == "o":
                    need = (("A", h, kind, a, b), 2)
                elif s == "M" and kind == "ret":
                    need = (("M", 1 - h, "go", fb, fa), 3)
                elif s == "B" and a != "i":
                    need = (("M", 1 - h, kind, fa, fb), 2 - delay)
                elif s == "B" and kind == "ret":
                    need = (("A", h, "go", b, a), 3 - delay)
                if need is not None and need[0] not in place:
                    break
                size = rows_of(h, a, b) if kind == "go" else rows_of(h, b, a)
                first = end[(s, h)]
                if need is not None:
                    ready = place[need[0]][0] + block * need[1]
                    first = jnp.where(size > 0, jnp.maximum(first, ready), first)
                place[(s, h, kind, a, b)] = (first, size)
                end[(s, h)] = first + size
                runs.pop(0)
    return place, end


def stream_kernel(
    n, dps, capacity, block, near_blocks, far_blocks, go_blocks, delay,
    row_ids, tok_hbm, gate_hbm, up_hbm, down_hbm,
    out_ref, slot_ref, flag_ref,
    gate_ref, up_ref, down_ref, pool, inbox, outbox,
    tok_key, in_key, position, counts, count_all, totals, total_all,
    tok_sem, own_sem, pair_send, pair_recv, near_send, near_recv, far_send, far_recv,
    count_send, count_recv, total_send, total_recv,
):
    me = lax.axis_index("expert")
    group = lax.axis_index("dp")
    tok = row_ids.shape[1]
    width = pool.shape[1]
    hidden = gate_ref.shape[2]
    core = lax.rem(me, 2)
    chip = lax.div(me, 2)
    half = lax.div(chip, 2)
    roles = {"o": 3 * half, "i": 1 + half, "p": 2 - half, "q": 3 - 3 * half}
    inner = chip == roles["i"]
    is_inner = inner.astype(jnp.int32)
    is_outer = 1 - is_inner
    near_dev = me + 2 - 4 * lax.rem(chip, 2)
    far_dev = 2 * (3 - chip) + core
    pair_dev = me + 1 - 2 * core
    two = 2 * block
    blocks = inbox.shape[0] // two
    steps = max(far_blocks, near_blocks + delay)
    local_at = tok + blocks * two
    piece = min(width, 512)
    ring = outbox.shape[0]

    def iota(shape, axis):
        return lax.broadcasted_iota(jnp.int32, shape, axis)

    def ones(mask):
        return mask.astype(F32).astype(BF16)

    def dot(a, b):
        return jnp.dot(a, b, preferred_element_type=F32)

    load_tok = pltpu.make_async_copy(tok_hbm, pool.at[pl.ds(0, tok)], tok_sem.at[0])
    load_tok.start()
    mine_down = pl.ds(pl.multiple_of(core * hidden, hidden), hidden)
    pairs = (
        (gate_hbm, gate_ref.at[core]), (up_hbm, up_ref.at[core]),
        (down_hbm, down_ref.at[mine_down]),
    )
    own = [
        pltpu.make_async_copy(src.at[0], dst, own_sem.at[i])
        for i, (src, dst) in enumerate(pairs)
    ]
    share = [
        pltpu.make_async_remote_copy(
            src_ref=src.at[0], dst_ref=dst, send_sem=pair_send.at[i],
            recv_sem=pair_recv.at[i], device_id={"expert": pair_dev}, device_id_type=MESH,
        )
        for i, (src, dst) in enumerate(pairs)
    ]
    other_down = pl.ds(pl.multiple_of((1 - core) * hidden, hidden), hidden)
    arriving = [
        pltpu.make_async_remote_copy(
            src_ref=src.at[0], dst_ref=dst, send_sem=pair_send.at[i],
            recv_sem=pair_recv.at[i], device_id={"expert": pair_dev}, device_id_type=MESH,
        )
        for i, (src, dst) in enumerate((
            (gate_hbm, gate_ref.at[1 - core]), (up_hbm, up_ref.at[1 - core]),
            (down_hbm, down_ref.at[other_down]),
        ))
    ]
    for copy in own:
        copy.start()

    barrier = pltpu.get_barrier_semaphore()

    def greet(i, c):
        pl.semaphore_signal(
            barrier, inc=1, device_id={"expert": lax.rem(me + i, n)}, device_id_type=MESH
        )
        return c

    def greet_dp(i, c):
        pl.semaphore_signal(
            barrier, inc=1, device_id={"dp": lax.rem(group + i, dps)}, device_id_type=MESH
        )
        return c

    lax.fori_loop(1, n, greet, 0)
    lax.fori_loop(1, dps, greet_dp, 0)

    ids_row = row_ids[...]
    hot_row = (ids_row == iota((n, tok), 0)).astype(F32)
    before_row = dot(hot_row.astype(BF16), ones(iota((tok, tok), 0) < iota((tok, tok), 1)))
    rank_row = jnp.sum(before_row * hot_row, axis=0, keepdims=True).astype(jnp.int32)
    mine = jnp.broadcast_to(jnp.sum(hot_row, axis=1, keepdims=True), (n, LANES))
    counts[...] = mine.astype(jnp.int32)
    row8 = iota((n, n), 0)
    shift = ones((iota((n, n), 1) + 1 == row8) & (lax.rem(row8, 2) == 1))
    skip = dot(shift, mine.astype(BF16))
    pair_rank = rank_row + jnp.sum(
        hot_row * skip[:, 0:1], axis=0, keepdims=True
    ).astype(jnp.int32)
    pair_row = lax.shift_right_logical(ids_row, 1)

    def own_rows(role):
        e = 2 * roles[role]
        return (counts[pl.ds(e, 1), :] + counts[pl.ds(e + 1, 1), :])[:, 0:1]

    zero1 = jnp.zeros((1, 1), jnp.int32)
    to_o = jnp.where(inner, zero1, LOCAL_KEY)
    to_i = jnp.where(inner, LOCAL_KEY, own_rows("p") + own_rows("q"))
    to_p = jnp.where(inner, zero1 + FAR_KEY, 0)
    to_q = own_rows("p") + jnp.where(inner, FAR_KEY, 0)
    key = jnp.zeros((1, tok), jnp.int32)
    for role, base in (("o", to_o), ("i", to_i), ("p", to_p), ("q", to_q)):
        key = jnp.where(pair_row == roles[role], base + pair_rank, key)
    tok_key[...] = key

    def near_copy(j, slot):
        return pltpu.make_async_remote_copy(
            src_ref=outbox.at[slot, pl.ds(0, block)],
            dst_ref=inbox.at[pl.ds(pl.multiple_of(j * two, two), block)],
            send_sem=near_send.at[slot], recv_sem=near_recv.at[j],
            device_id={"expert": near_dev}, device_id_type=MESH,
        )

    def far_copy(j, slot):
        return pltpu.make_async_remote_copy(
            src_ref=outbox.at[slot, pl.ds(block, block)],
            dst_ref=inbox.at[pl.ds(pl.multiple_of(j * two + block, block), block)],
            send_sem=far_send.at[slot], recv_sem=far_recv.at[j],
            device_id={"expert": far_dev}, device_id_type=MESH,
        )

    def count(dest, source):
        return pltpu.make_async_remote_copy(
            src_ref=counts, dst_ref=count_all.at[source],
            send_sem=count_send.at[dest], recv_sem=count_recv.at[source],
            device_id={"expert": dest}, device_id_type=MESH,
        )

    def total(dest, source):
        return pltpu.make_async_remote_copy(
            src_ref=totals, dst_ref=total_all.at[source],
            send_sem=total_send.at[dest], recv_sem=total_recv.at[source],
            device_id={"dp": dest}, device_id_type=MESH,
        )

    def sent(k):
        slot = lax.rem(k, ring)
        near_at = k - delay * is_inner

        @pl.when((near_at >= 0) & (near_at < near_blocks))
        def _():
            near_copy(near_at, slot).wait_send()

        @pl.when(inner & (k < far_blocks))
        def _():
            far_copy(k, slot).wait_send()

    def send(k, low, high):
        slot = lax.rem(k, ring)
        near_at = k - delay * is_inner

        @pl.when(k >= ring)
        def _():
            sent(k - ring)

        @pl.when(inner | (k < near_blocks))
        def _():
            row = iota((two, 1), 0)
            want = jnp.where(
                row < block, near_at * block + row, FAR_KEY + k * block + row - block
            )
            picks = []
            if low < tok:
                picks.append(ones(want == tok_key[...]))
            if high > tok:
                picks.append(ones(want == in_key[:, max(low, tok) - tok : high - tok]))
            pick = picks[0] if len(picks) == 1 else jnp.concatenate(picks, axis=1)
            for at in range(0, width, piece):
                outbox[slot, :, at : at + piece] = dot(
                    pick, pool[low:high, at : at + piece]
                ).astype(BF16)

        @pl.when((near_at >= 0) & (near_at < near_blocks))
        def _():
            near_copy(near_at, slot).start()

        @pl.when(inner & (k < far_blocks))
        def _():
            far_copy(k, slot).start()

    def arrive(b):
        at = pl.multiple_of(b * two, two)

        @pl.when((b >= 0) & (b < near_blocks))
        def _():
            near_copy(b, 0).wait_recv()
            pool[pl.ds(tok + at, block), :] = inbox[pl.ds(at, block), :]

        @pl.when(inner & (b >= 0) & (b < far_blocks))
        def _():
            far_copy(b, 0).wait_recv()
            pool[pl.ds(tok + at + block, block), :] = inbox[pl.ds(at + block, block), :]

    def ffn(rows, code):
        parts = []
        wide = jnp.broadcast_to(code, (two, hidden))
        for parity in (0, 1):
            gate = dot(rows, gate_ref[parity])
            up = dot(rows, up_ref[parity])
            act = gate / (1.0 + jnp.exp(-gate)) * up
            parts.append(jnp.where(wide == parity + 1, act, 0.0).astype(BF16))
        act = jnp.concatenate(parts, axis=1)
        return [
            dot(act, down_ref[:, at : at + piece]) for at in range(0, width, piece)
        ]

    spare = pool.at[pl.ds(tok, blocks * two)]

    def clear(i, c):
        spare[pl.ds(pl.multiple_of(i * two, two), two), :] = jnp.zeros((two, width), BF16)
        return c

    lax.fori_loop(0, blocks, clear, 0)
    load_tok.wait()
    pl.semaphore_wait(barrier, n + dps - 2)

    def tell(i, c):
        count(lax.rem(me + i, n), me).start()
        return c

    lax.fori_loop(1, n, tell, 0)
    count_all[me] = counts[...]

    def first_steps(k, c):
        send(k, 0, tok)
        return c

    lax.fori_loop(0, 2, first_steps, 0)
    for copy in share:
        copy.start()

    def heard(i, c):
        count(me, lax.rem(me + i, n)).wait_recv()
        return c

    lax.fori_loop(1, n, heard, 0)

    def rows_of(lane):
        def get(h, a, b):
            a, b = (FLIP[a], FLIP[b]) if h else (a, b)
            dev, e = 2 * roles[a] + lane, 2 * roles[b]
            return count_all[dev, pl.ds(e, 1), :] + count_all[dev, pl.ds(e + 1, 1), :]

        return get

    def even(a):
        return count_all[2 * roles[a] + core, pl.ds(2 * chip, 1), :][:, 0:1]

    place, ends = lay_streams(rows_of(core), block, delay)
    over = jnp.zeros((1, LANES), jnp.int32)
    for lane_place, lane_ends in (
        (place, ends), lay_streams(rows_of(1 - core), block, delay)
    ):
        for (s, _), end in lane_ends.items():
            limit = (far_blocks if s == "M" else near_blocks) * block
            over = jnp.maximum(over, (end > limit).astype(jnp.int32))
        for name, (first, size) in lane_place.items():
            if name[2] == "go":
                late = (first + size > go_blocks * block) & (size > 0)
                over = jnp.maximum(over, late.astype(jnp.int32))

    def at(name):
        first, size = place[name]
        return first[:, 0:1], size[:, 0:1]

    def choose(a, b):
        return tuple(jnp.where(inner, x, y) for x, y in zip(at(a), at(b)))

    def start(name):
        return at(name)[0]

    lane = iota((1, blocks * two), 1)
    inside = lax.rem(lane, two)
    is_far = inside >= block
    spot = lax.div(lane, two) * block + lax.rem(inside, block)
    nowhere = zero1 - 65536
    code = jnp.full((1, blocks * two), -1, jnp.int32)
    near_runs = (
        (("A", 0, "go", "o", "p"), ("B", 0, "go", "i", "o"),
         FAR_KEY + start(("M", 0, "go", "o", "p")), start(("A", 0, "ret", "o", "i"))),
        (("A", 0, "go", "o", "q"), ("B", 0, "go", "p", "o"),
         FAR_KEY + start(("M", 0, "go", "o", "q")), start(("A", 0, "ret", "o", "p"))),
        (("A", 0, "go", "o", "i"), ("B", 0, "go", "q", "o"),
         start(("B", 0, "ret", "i", "o")), start(("A", 0, "ret", "o", "q"))),
        (("A", 0, "ret", "o", "p"), ("B", 0, "ret", "p", "o"),
         FAR_KEY + start(("M", 0, "ret", "o", "p")), nowhere),
        (("A", 0, "ret", "o", "q"), ("B", 0, "ret", "q", "o"),
         FAR_KEY + start(("M", 0, "ret", "o", "q")), nowhere),
    )
    for in_run, out_run, to_in, to_out in near_runs:
        first, size = choose(in_run, out_run)
        to = jnp.where(inner, to_in, to_out)
        hit = (spot >= first) & (spot < first + size) & jnp.logical_not(is_far)
        code = jnp.where(hit, spot + (to - first), code)
    far_runs = (
        (("M", 1, "go", "i", "p"), FAR_KEY + start(("M", 0, "ret", "i", "p"))),
        (("M", 1, "go", "i", "q"), start(("B", 0, "go", "p", "o"))),
        (("M", 1, "go", "o", "p"), FAR_KEY + start(("M", 0, "ret", "i", "q"))),
        (("M", 1, "go", "o", "q"), start(("B", 0, "go", "q", "o"))),
        (("M", 1, "ret", "i", "q"), start(("B", 0, "ret", "p", "o"))),
        (("M", 1, "ret", "o", "q"), start(("B", 0, "ret", "q", "o"))),
    )
    for run, to in far_runs:
        first, size = at(run)
        hit = (spot >= first) & (spot < first + size) & is_far
        code = jnp.where(hit, spot + (to - first), code)
    in_key[...] = code

    mine_runs = []
    for in_run, out_run, far_side, a_in, a_out in (
        (("A", 0, "go", "o", "i"), ("B", 0, "go", "i", "o"), 0, "o", "i"),
        (("M", 1, "go", "i", "p"), ("B", 0, "go", "p", "o"), 1, "p", "p"),
        (("M", 1, "go", "o", "p"), ("B", 0, "go", "q", "o"), 1, "q", "q"),
    ):
        first, size = choose(in_run, out_run)
        split = jnp.where(inner, even(a_in), even(a_out))
        mine_runs.append((first, size, split, far_side * is_inner))

    def mark(b):
        row = iota((two, 1), 0)
        side = lax.div(row, block)
        spot = b * block + lax.rem(row, block)
        code = jnp.zeros((two, 1), jnp.int32)
        for first, size, split, which in mine_runs:
            hit = (spot >= first) & (spot < first + size) & (side == which)
            code = jnp.where(hit, jnp.where(spot - first >= split, 2, 1), code)
        return code

    home = zero1 + local_at

    def pool_at(run, side):
        def get(rank):
            spot = start(run) + rank
            return (
                tok + lax.div(spot, block) * two + lax.rem(spot, block) + side * block
            )

        return get

    back_in = {
        "o": pool_at(("A", 0, "ret", "o", "i"), 0),
        "p": pool_at(("M", 1, "ret", "i", "p"), 1),
        "q": pool_at(("M", 1, "ret", "o", "p"), 1),
        "i": lambda rank: home + rank,
    }
    back_out = {
        "i": pool_at(("B", 0, "ret", "i", "o"), 0),
        "p": pool_at(("B", 0, "ret", "p", "o"), 0),
        "q": pool_at(("B", 0, "ret", "q", "o"), 0),
        "o": lambda rank: home + rank,
    }
    from_row = jnp.zeros((1, tok), jnp.int32)
    for role in "oipq":
        found = jnp.where(inner, back_in[role](pair_rank), back_out[role](pair_rank))
        from_row = jnp.where(pair_row == roles[role], found, from_row)

    def add(i, carry):
        before, whole = carry
        here = count_all[i]
        return before + here * (i < me).astype(jnp.int32), whole + here

    zero = jnp.zeros((n, LANES), jnp.int32)
    before, whole = lax.fori_loop(0, n, add, (zero, zero))
    over = jnp.broadcast_to(over, (n, LANES))
    totals[0] = whole
    totals[1] = over
    total_all[group, 0] = whole
    total_all[group, 1] = over

    def tell_dp(i, c):
        total(lax.rem(group + i, dps), group).start()
        return c

    lax.fori_loop(1, dps, tell_dp, 0)

    def work(b):
        at = pl.multiple_of(tok + b * two, two)
        code = mark(b)
        done = ffn(pool[pl.ds(at, two), :], code)
        wide = jnp.broadcast_to(code, (two, piece))
        for i, part in enumerate(done):
            cols = slice(i * piece, (i + 1) * piece)
            raw = pool[pl.ds(at, two), cols].astype(F32)
            pool[pl.ds(at, two), cols] = jnp.where(wide > 0, part, raw).astype(BF16)

    def step(low, high, busy):
        def run(k, c):
            b = k - 2 - delay * is_outer
            arrive(b)
            send(k, low, high)
            if busy:
                @pl.when((b >= 0) & (b < go_blocks))
                def _():
                    work(b)

            return c

        return run

    def local(i, c):
        rank = i * two + iota((two, 1), 0)
        rows = dot(ones(rank + LOCAL_KEY == tok_key[...]), pool[0:tok, :]).astype(BF16)
        e = 2 * chip
        first = counts[pl.ds(e, 1), :][:, 0:1]
        both = first + counts[pl.ds(e + 1, 1), :][:, 0:1]
        code = jnp.where(rank < both, jnp.where(rank >= first, 2, 1), 0)
        at = pl.multiple_of(local_at + i * two, two)
        for j, part in enumerate(ffn(rows, code)):
            pool[pl.ds(at, two), j * piece : (j + 1) * piece] = part.astype(BF16)
        return c

    cut = tok // block
    last = go_blocks + 2 + delay
    lax.fori_loop(2, 3, step(0, tok + two, False), 0)
    for copy in own:
        copy.wait()
    for copy in arriving:
        copy.wait_recv()

    @pl.when(inner)
    def _():
        work(0)

    lax.fori_loop(3, cut, step(0, tok + (cut - 2) * two, True), 0)
    lax.fori_loop(cut, last, step(tok, tok + (last - 2) * two, True), 0)
    lax.fori_loop(last, steps, step(tok, local_at, False), 0)
    lax.fori_loop(0, 2, local, 0)

    def heard_dp(i, c):
        total(group, lax.rem(group + i, dps)).wait_recv()
        return c

    lax.fori_loop(1, dps, heard_dp, 0)

    def add_dp(i, carry):
        outer, most = carry
        return (
            outer + total_all[i, 0] * (i < group).astype(jnp.int32),
            jnp.maximum(most, total_all[i, 1]),
        )

    outer, most = lax.fori_loop(0, dps, add_dp, (zero, over))
    offset = before + outer
    flag_ref[...] = most
    slot = jnp.sum(
        hot_row * offset[:, 0:1].astype(F32), axis=0, keepdims=True
    ).astype(jnp.int32) + rank_row
    slot_ref[...] = slot
    from_row = jnp.where(slot < capacity, from_row, 0)
    position[...] = jnp.transpose(
        jnp.broadcast_to(from_row, (8, tok)).astype(F32)
    )[:, 0:1].astype(jnp.int32)

    span = 4 * two

    def combine(at, size, first):
        pick = ones(position[...] == iota((1, size), 1) + at)
        rows = pl.ds(at if isinstance(at, int) else pl.multiple_of(at, two), size)
        for col in range(0, width, piece):
            part = dot(pick, pool[rows, col : col + piece]).astype(BF16)
            if first:
                out_ref[:, col : col + piece] = part
            else:
                out_ref[:, col : col + piece] += part

    seen = (steps - 2 - delay) * two // span
    combine(tok, span, True)

    def combine_step(c, carry):
        combine(tok + c * span, span, False)
        return carry

    lax.fori_loop(1, seen, combine_step, 0)

    def late(b, c):
        arrive(b)
        return c

    lax.fori_loop(steps - 2 - delay * is_outer, near_blocks, late, 0)
    rest = tok + seen * span
    combine(rest, pool.shape[0] - rest, False)

    def flush(k, c):
        sent(k)
        return c

    lax.fori_loop(steps - ring, steps, flush, 0)
    for copy in share:
        copy.wait_send()

    def drain(i, c):
        count(lax.rem(me + i, n), me).wait_send()
        return c

    lax.fori_loop(1, n, drain, 0)

    def drain_dp(i, c):
        total(lax.rem(group + i, dps), group).wait_send()
        return c

    lax.fori_loop(1, dps, drain_dp, 0)


def streamed(tokens, expert_ids, gate_proj, up_proj, down_proj):
    tok, width = tokens.shape
    hidden = gate_proj.shape[2]
    n = lax.axis_size("expert")
    dps = lax.axis_size("dp")
    capacity = tok * dps
    block = tok // n
    near_blocks, far_blocks, go_blocks, delay = NEAR_BLOCKS, FAR_BLOCKS, GO_BLOCKS, DELAY
    blocks = max(near_blocks, far_blocks)
    ring = 4
    vmem = pl.BlockSpec(memory_space=pltpu.VMEM)
    anywhere = pl.BlockSpec(memory_space=pltpu.MemorySpace.HBM)
    dma = pltpu.SemaphoreType.DMA
    table = pltpu.VMEM((n, LANES), jnp.int32)
    mixed, slot, flag = pl.pallas_call(
        functools.partial(
            stream_kernel, n, dps, capacity, block, near_blocks, far_blocks, go_blocks, delay
        ),
        out_shape=(
            jax.ShapeDtypeStruct((tok, width), BF16),
            jax.ShapeDtypeStruct((1, tok), jnp.int32),
            jax.ShapeDtypeStruct((n, LANES), jnp.int32),
        ),
        in_specs=[vmem, anywhere, anywhere, anywhere, anywhere],
        out_specs=(vmem, vmem, vmem),
        scratch_shapes=[
            pltpu.VMEM((2, width, hidden), BF16),
            pltpu.VMEM((2, width, hidden), BF16),
            pltpu.VMEM((2 * hidden, width), BF16),
            pltpu.VMEM((tok + 2 * block * blocks + 4 * block, width), BF16),
            pltpu.VMEM((2 * block * blocks, width), BF16),
            pltpu.VMEM((ring, 2 * block, width), BF16),
            pltpu.VMEM((1, tok), jnp.int32),
            pltpu.VMEM((1, 2 * block * blocks), jnp.int32),
            pltpu.VMEM((tok, 1), jnp.int32),
            table,
            pltpu.VMEM((n, n, LANES), jnp.int32),
            pltpu.VMEM((2, n, LANES), jnp.int32),
            pltpu.VMEM((dps, 2, n, LANES), jnp.int32),
            dma((1,)), dma((3,)), dma((3,)), dma((3,)),
            dma((ring,)), dma((near_blocks,)), dma((ring,)), dma((far_blocks,)),
            dma((n,)), dma((n,)), dma((dps,)), dma((dps,)),
        ],
        compiler_params=pltpu.CompilerParams(
            collective_id=0, has_side_effects=True, vmem_limit_bytes=60 * 2**20
        ),
    )(expert_ids.reshape(1, tok), tokens, gate_proj, up_proj, down_proj)
    return lax.cond(
        flag[0, 0] > 0,
        lambda: padded(tokens, expert_ids, gate_proj, up_proj, down_proj),
        lambda: (mixed, slot.reshape(tok)),
    )


def on_device(tokens, expert_ids, gate_proj, up_proj, down_proj):
    n = lax.axis_size("expert")
    if n == 8 and tokens.shape[0] // n % 64 == 0:
        return streamed(tokens, expert_ids, gate_proj, up_proj, down_proj)
    return direct(tokens, expert_ids, gate_proj, up_proj, down_proj)


def solution(mesh):
    in_specs = (
        P(("dp", "expert"), None),
        P(("dp", "expert"), None),
        P("expert", None, None),
        P("expert", None, None),
        P("expert", None, None),
    )
    out_specs = (P(("dp", "expert"), None), P(("dp", "expert")))
    return jax.shard_map(
        on_device, mesh=mesh, in_specs=in_specs, out_specs=out_specs, check_vma=False
    )
```

```python
import functools

import jax
import jax.numpy as jnp
from jax import lax
from jax.experimental import pallas as pl
from jax.experimental.pallas import tpu as pltpu
from jax.sharding import PartitionSpec as P

MESH = pl.DeviceIdType.MESH
F32 = jnp.float32
BF16 = jnp.bfloat16
LANES = 128
LAG, HOLD = 3, 9


def spread(step, n):
    half = (step // 2) * (2 * (step % 2) - 1)
    return jnp.where(step == 0, 0, n // 2 + half)


def direct_kernel(
    n, dps, most, capacity,
    row_ids, col_ids, tok_ref, gate_hbm, up_hbm, down_hbm,
    out_ref, slot_ref,
    gate_ref, up_ref, down_ref, outgoing, arrived, results, returned,
    position, offset, counts, count_all, totals, total_all,
    weight_sem, go_send, go_recv, back_send, back_recv,
    count_send, count_recv, total_send, total_recv,
):
    me = lax.axis_index("expert")
    group = lax.axis_index("dp")
    tok = tok_ref.shape[0]
    width = tok_ref.shape[1]

    weights = [
        pltpu.make_async_copy(src.at[0], dst, weight_sem.at[i])
        for i, (src, dst) in enumerate(
            ((gate_hbm, gate_ref), (up_hbm, up_ref), (down_hbm, down_ref))
        )
    ]
    for copy in weights:
        copy.start()

    barrier = pltpu.get_barrier_semaphore()

    def greet(i, c):
        pl.semaphore_signal(
            barrier, inc=1, device_id={"expert": lax.rem(me + i, n)}, device_id_type=MESH
        )
        return c

    def greet_dp(i, c):
        pl.semaphore_signal(
            barrier, inc=1, device_id={"dp": lax.rem(group + i, dps)}, device_id_type=MESH
        )
        return c

    lax.fori_loop(1, n, greet, 0)
    lax.fori_loop(1, dps, greet_dp, 0)

    earlier = lax.broadcasted_iota(jnp.int32, (tok, tok), 0) < lax.broadcasted_iota(
        jnp.int32, (tok, tok), 1
    )
    later = lax.broadcasted_iota(jnp.int32, (tok, tok), 0) > lax.broadcasted_iota(
        jnp.int32, (tok, tok), 1
    )
    ids_row = row_ids[...]
    hot_row = (ids_row == lax.broadcasted_iota(jnp.int32, (n, tok), 0)).astype(F32)
    before_row = jnp.dot(
        hot_row.astype(BF16), earlier.astype(F32).astype(BF16), preferred_element_type=F32
    )
    rank_row = jnp.sum(before_row * hot_row, axis=0, keepdims=True).astype(jnp.int32)
    pos_row = ids_row * most + rank_row
    counts[...] = jnp.broadcast_to(
        jnp.sum(hot_row, axis=1, keepdims=True), (n, LANES)
    ).astype(jnp.int32)

    ids_col = col_ids[...]
    hot_col = (ids_col == lax.broadcasted_iota(jnp.int32, (tok, n), 1)).astype(F32)
    before_col = jnp.dot(
        later.astype(F32).astype(BF16), hot_col.astype(BF16), preferred_element_type=F32
    )
    rank_col = jnp.sum(before_col * hot_col, axis=1, keepdims=True).astype(jnp.int32)
    position[...] = ids_col * most + rank_col

    def go(dest, source):
        return pltpu.make_async_remote_copy(
            src_ref=outgoing.at[dest], dst_ref=arrived.at[source],
            send_sem=go_send.at[dest], recv_sem=go_recv.at[source],
            device_id={"expert": dest}, device_id_type=MESH,
        )

    def back(dest, source):
        return pltpu.make_async_remote_copy(
            src_ref=results.at[dest], dst_ref=returned.at[source],
            send_sem=back_send.at[dest], recv_sem=back_recv.at[source],
            device_id={"expert": dest}, device_id_type=MESH,
        )

    def count(dest, source):
        return pltpu.make_async_remote_copy(
            src_ref=counts, dst_ref=count_all.at[source],
            send_sem=count_send.at[dest], recv_sem=count_recv.at[source],
            device_id={"expert": dest}, device_id_type=MESH,
        )

    def total(dest, source):
        return pltpu.make_async_remote_copy(
            src_ref=totals, dst_ref=total_all.at[source],
            send_sem=total_send.at[dest], recv_sem=total_recv.at[source],
            device_id={"dp": dest}, device_id_type=MESH,
        )

    def pack(dest):
        pick = (
            lax.broadcasted_iota(jnp.int32, (most, tok), 0) + dest * most == pos_row
        ).astype(F32).astype(BF16)
        return jnp.dot(pick, tok_ref[...], preferred_element_type=F32).astype(BF16)

    pl.semaphore_wait(barrier, n + dps - 2)

    def dispatch(i, c):
        dest = lax.rem(me + spread(i, n), n)
        outgoing[dest] = pack(dest)
        go(dest, me).start()
        return c

    lax.fori_loop(1, n, dispatch, 0)

    def tell(i, c):
        count(lax.rem(me + i, n), me).start()
        return c

    lax.fori_loop(1, n, tell, 0)
    count_all[me] = counts[...]
    arrived[me] = pack(me)

    for copy in weights:
        copy.wait()

    def ffn(source):
        rows = arrived[source]
        gate = jnp.dot(rows, gate_ref[...], preferred_element_type=F32)
        up = jnp.dot(rows, up_ref[...], preferred_element_type=F32)
        hidden = (gate / (1.0 + jnp.exp(-gate)) * up).astype(BF16)
        return jnp.dot(hidden, down_ref[...], preferred_element_type=F32).astype(BF16)

    def expert_step(i, c):
        source = lax.rem(me + n - spread(i, n), n)

        @pl.when(i > 0)
        def _():
            go(me, source).wait_recv()

        results[source] = ffn(source)

        @pl.when(i > 0)
        def _():
            back(source, me).start()

        return c

    lax.fori_loop(0, n, expert_step, 0)

    def heard(i, c):
        count(me, lax.rem(me + i, n)).wait_recv()
        return c

    lax.fori_loop(1, n, heard, 0)

    def add(i, carry):
        inner, whole = carry
        here = count_all[i]
        return inner + here * (i < me).astype(jnp.int32), whole + here

    zero = jnp.zeros((n, LANES), jnp.int32)
    inner, whole = lax.fori_loop(0, n, add, (zero, zero))
    totals[...] = whole

    def tell_dp(i, c):
        total(lax.rem(group + i, dps), group).start()
        return c

    lax.fori_loop(1, dps, tell_dp, 0)
    total_all[group] = whole

    def heard_dp(i, c):
        total(group, lax.rem(group + i, dps)).wait_recv()
        return c

    lax.fori_loop(1, dps, heard_dp, 0)

    def add_dp(i, outer):
        return outer + total_all[i] * (i < group).astype(jnp.int32)

    offset[...] = inner + lax.fori_loop(0, dps, add_dp, zero)
    slot_ref[...] = (
        jnp.sum(
            hot_row * offset[:, 0:1].astype(F32), axis=0, keepdims=True
        ).astype(jnp.int32)
        + rank_row
    )

    piece = min(width, 512)

    def combine(source, block, first):
        lane = lax.broadcasted_iota(jnp.int32, (tok, most), 1)
        fits = offset[pl.ds(source, 1), 0:most] + lax.broadcasted_iota(
            jnp.int32, (1, most), 1
        ) < capacity
        pick = (lane + source * most == position[...]) & fits
        pick = pick.astype(F32).astype(BF16)
        for at in range(0, width, piece):
            part = jnp.dot(
                pick, block[source, :, at : at + piece], preferred_element_type=F32
            ).astype(BF16)
            if first:
                out_ref[:, at : at + piece] = part
            else:
                out_ref[:, at : at + piece] += part

    combine(me, results, True)

    def combine_step(i, c):
        source = lax.rem(me + n - spread(i, n), n)
        back(me, source).wait_recv()
        combine(source, returned, False)
        return c

    lax.fori_loop(1, n, combine_step, 0)

    def drain(i, c):
        other = lax.rem(me + i, n)
        go(other, me).wait_send()
        back(other, me).wait_send()
        count(other, me).wait_send()
        return c

    lax.fori_loop(1, n, drain, 0)

    def drain_dp(i, c):
        total(lax.rem(group + i, dps), group).wait_send()
        return c

    lax.fori_loop(1, dps, drain_dp, 0)


def direct(tokens, expert_ids, gate_proj, up_proj, down_proj):
    tok, width = tokens.shape
    hidden = gate_proj.shape[2]
    n = lax.axis_size("expert")
    dps = lax.axis_size("dp")
    most = 2 * tok // n
    capacity = tok * dps
    vmem = pl.BlockSpec(memory_space=pltpu.VMEM)
    anywhere = pl.BlockSpec(memory_space=pltpu.MemorySpace.HBM)
    dma = pltpu.SemaphoreType.DMA
    block = pltpu.VMEM((n, most, width), BF16)
    mixed, slot = pl.pallas_call(
        functools.partial(direct_kernel, n, dps, most, capacity),
        out_shape=(
            jax.ShapeDtypeStruct((tok, width), BF16),
            jax.ShapeDtypeStruct((1, tok), jnp.int32),
        ),
        in_specs=[vmem, vmem, vmem, anywhere, anywhere, anywhere],
        out_specs=(vmem, vmem),
        scratch_shapes=[
            pltpu.VMEM((width, hidden), BF16),
            pltpu.VMEM((width, hidden), BF16),
            pltpu.VMEM((hidden, width), BF16),
            block, block, block, block,
            pltpu.VMEM((tok, 1), jnp.int32),
            pltpu.VMEM((n, LANES), jnp.int32),
            pltpu.VMEM((n, LANES), jnp.int32),
            pltpu.VMEM((n, n, LANES), jnp.int32),
            pltpu.VMEM((n, LANES), jnp.int32),
            pltpu.VMEM((dps, n, LANES), jnp.int32),
            dma((3,)), dma((n,)), dma((n,)), dma((n,)), dma((n,)),
            dma((n,)), dma((n,)), dma((dps,)), dma((dps,)),
        ],
        compiler_params=pltpu.CompilerParams(
            collective_id=0, has_side_effects=True, vmem_limit_bytes=60 * 2**20
        ),
    )(
        expert_ids.reshape(1, tok), expert_ids, tokens, gate_proj, up_proj, down_proj
    )
    return mixed, slot.reshape(tok)


def entering(part, axis, combine, identity):
    place = lax.axis_index(axis)
    gathered = lax.all_gather(part, axis)
    state = jnp.zeros_like(part) + jnp.asarray(identity, part.dtype)

    def one(hop, state):
        return combine(state, lax.dynamic_index_in_dim(gathered, hop, 0, False))

    return lax.fori_loop(0, place, one, state)


def add_counts(earlier, later):
    return earlier + later


def expert_ffn(rows, gate_proj, up_proj, down_proj):
    gate_val = jnp.dot(rows, gate_proj[0], preferred_element_type=jnp.float32)
    up_val = jnp.dot(rows, up_proj[0], preferred_element_type=jnp.float32)
    hidden = (jax.nn.silu(gate_val) * up_val).astype(jnp.bfloat16)
    return jnp.dot(hidden, down_proj[0], preferred_element_type=jnp.float32).astype(jnp.bfloat16)


def padded(tokens, expert_ids, gate_proj, up_proj, down_proj):
    tok_rows, width = tokens.shape
    experts_all = lax.axis_size("expert")
    most = 2 * tok_rows // experts_all
    capacity = tok_rows * lax.axis_size("dp")
    choices = expert_ids[:, 0]
    onehot = (choices[:, None] == jnp.arange(experts_all, dtype=jnp.int32)[None, :]).astype(
        jnp.int32
    )
    counts = jnp.sum(onehot, axis=0)
    inner = entering(counts, "expert", add_counts, jnp.zeros_like(counts))
    totals = lax.psum(counts, "expert")
    outer = entering(totals, "dp", add_counts, jnp.zeros_like(totals))
    offset = inner + outer
    before = jnp.cumsum(onehot, axis=0) - onehot
    local_rank = jnp.sum(before * onehot, axis=1)
    global_slot = (jnp.sum(onehot * offset[None, :], axis=1) + local_rank).astype(jnp.int32)
    is_kept = global_slot < capacity
    position = choices * most + local_rank
    targets = jnp.arange(experts_all * most, dtype=jnp.int32)
    dispatch = ((targets[:, None] == position[None, :]) & is_kept[None, :]).astype(jnp.bfloat16)
    outgoing = jnp.dot(dispatch, tokens, preferred_element_type=jnp.float32).astype(jnp.bfloat16)
    outgoing = outgoing.reshape(experts_all, most, width)
    arrived = lax.all_to_all(outgoing, "expert", split_axis=0, concat_axis=0, tiled=True)
    sources, slots_here, _ = arrived.shape
    flat = arrived.reshape(sources * slots_here, width)
    returned = lax.all_to_all(
        expert_ffn(flat, gate_proj, up_proj, down_proj).reshape(sources, slots_here, width),
        "expert",
        split_axis=0,
        concat_axis=0,
        tiled=True,
    )
    flat_back = returned.reshape(experts_all * most, width)
    mixed = lax.dot_general(
        dispatch, flat_back, (((0,), (0,)), ((), ())), preferred_element_type=jnp.float32
    )
    return (mixed.astype(jnp.bfloat16), global_slot)


RUN_ORDER = {
    "A": ("go op", "go oq", "go oi", "ret op", "ret oq", "ret oi"),
    "M": (
        "go ip", "go iq", "go oq", "go op", "ret ip", "ret op", "ret iq", "ret oq",
    ),
    "B": ("go io", "go po", "go qo", "ret io", "ret po", "ret qo"),
}
FLIP = {"o": "q", "i": "p", "p": "i", "q": "o"}
FAR_KEY = 4096
LOCAL_KEY = 8192


def lay_streams(rows_of, block):
    place, end = {}, {}
    queue = {
        (s, h): [(run[:-3], run[-2], run[-1]) for run in RUN_ORDER[s]]
        for s in "AMB" for h in (0, 1)
    }
    zero = jnp.zeros((1, LANES), jnp.int32)
    for name in queue:
        end[name] = zero
    while any(queue.values()):
        for (s, h), runs in queue.items():
            while runs:
                kind, a, b = runs[0]
                fa, fb = FLIP[a], FLIP[b]
                need, result = None, kind == "ret"
                if s == "A" and kind == "ret":
                    need = ("B", h, "go", b, a)
                elif s == "M" and a == "o":
                    need, result = ("A", h, kind, a, b), False
                elif s == "M" and kind == "ret":
                    need = ("M", 1 - h, "go", fb, fa)
                elif s == "B" and a != "i":
                    need, result = ("M", 1 - h, kind, fa, fb), False
                elif s == "B" and kind == "ret":
                    need = ("A", h, "go", b, a)
                if need is not None and need not in place:
                    break
                size = rows_of(h, a, b) if kind == "go" else rows_of(h, b, a)
                first = end[(s, h)]
                if need is not None:
                    there = place[need][0]
                    ready = there + block * LAG
                    if result:
                        ready = jnp.maximum(
                            ready + block * 2,
                            lax.shift_right_logical(there, 1) + block * (HOLD + 1),
                        )
                    first = jnp.where(size > 0, jnp.maximum(first, ready), first)
                place[(s, h, kind, a, b)] = (first, size)
                end[(s, h)] = first + size
                runs.pop(0)
    return place, end


def stream_kernel(
    n, dps, capacity, block, near_blocks, far_blocks, go_blocks, back_blocks,
    row_ids, tok_hbm, gate_hbm, up_hbm, down_hbm,
    out_ref, slot_ref, flag_ref,
    gate_ref, up_ref, down_ref, pool, inbox, outbox,
    tok_key, in_key, position, counts, count_all, totals, total_all,
    tok_sem, own_sem, pair_send, pair_recv, near_send, near_recv, far_send, far_recv,
    count_send, count_recv, total_send, total_recv,
):
    me = lax.axis_index("expert")
    group = lax.axis_index("dp")
    tok = row_ids.shape[1]
    width = pool.shape[1]
    hidden = gate_ref.shape[2]
    core = lax.rem(me, 2)
    chip = lax.div(me, 2)
    half = lax.div(chip, 2)
    roles = {"o": 3 * half, "i": 1 + half, "p": 2 - half, "q": 3 - 3 * half}
    inner = chip == roles["i"]
    is_inner = inner.astype(jnp.int32)
    near_limit = near_blocks - LAG * (1 - is_inner)
    near_dev = me + 2 - 4 * lax.rem(chip, 2)
    far_dev = 2 * (3 - chip) + core
    pair_dev = me + 1 - 2 * core
    two = 2 * block
    blocks = inbox.shape[0] // two
    pair = 2 * two
    steps = near_blocks
    tok_at = 2 * pair
    base = tok_at + tok
    piece = min(width, 512)
    ring = outbox.shape[0]

    def iota(shape, axis):
        return lax.broadcasted_iota(jnp.int32, shape, axis)

    def ones(mask):
        return mask.astype(F32).astype(BF16)

    def dot(a, b):
        return jnp.dot(a, b, preferred_element_type=F32)

    load_tok = pltpu.make_async_copy(tok_hbm, pool.at[pl.ds(tok_at, tok)], tok_sem.at[0])
    load_tok.start()
    mine_down = pl.ds(pl.multiple_of(core * hidden, hidden), hidden)
    pairs = (
        (gate_hbm, gate_ref.at[core]), (up_hbm, up_ref.at[core]),
        (down_hbm, down_ref.at[mine_down]),
    )
    own = [
        pltpu.make_async_copy(src.at[0], dst, own_sem.at[i])
        for i, (src, dst) in enumerate(pairs)
    ]
    share = [
        pltpu.make_async_remote_copy(
            src_ref=src.at[0], dst_ref=dst, send_sem=pair_send.at[i],
            recv_sem=pair_recv.at[i], device_id={"expert": pair_dev}, device_id_type=MESH,
        )
        for i, (src, dst) in enumerate(pairs)
    ]
    other_down = pl.ds(pl.multiple_of((1 - core) * hidden, hidden), hidden)
    arriving = [
        pltpu.make_async_remote_copy(
            src_ref=src.at[0], dst_ref=dst, send_sem=pair_send.at[i],
            recv_sem=pair_recv.at[i], device_id={"expert": pair_dev}, device_id_type=MESH,
        )
        for i, (src, dst) in enumerate((
            (gate_hbm, gate_ref.at[1 - core]), (up_hbm, up_ref.at[1 - core]),
            (down_hbm, down_ref.at[other_down]),
        ))
    ]
    for copy in own:
        copy.start()

    barrier = pltpu.get_barrier_semaphore()

    def greet(i, c):
        pl.semaphore_signal(
            barrier, inc=1, device_id={"expert": lax.rem(me + i, n)}, device_id_type=MESH
        )
        return c

    def greet_dp(i, c):
        pl.semaphore_signal(
            barrier, inc=1, device_id={"dp": lax.rem(group + i, dps)}, device_id_type=MESH
        )
        return c

    lax.fori_loop(1, n, greet, 0)
    lax.fori_loop(1, dps, greet_dp, 0)

    ids_row = row_ids[...]
    hot_row = (ids_row == iota((n, tok), 0)).astype(F32)
    earlier = ones(iota((LANES, LANES), 0) < iota((LANES, LANES), 1))
    ahead, mine = [], jnp.zeros((n, 1), F32)
    for lo in range(0, tok, LANES):
        hot = hot_row[:, lo : lo + LANES]
        ahead.append(dot(hot.astype(BF16), earlier) + mine)
        mine = mine + jnp.sum(hot, axis=1, keepdims=True)
    before_row = jnp.concatenate(ahead, axis=1)
    rank_row = jnp.sum(before_row * hot_row, axis=0, keepdims=True).astype(jnp.int32)
    mine = jnp.broadcast_to(mine, (n, LANES))
    counts[...] = mine.astype(jnp.int32)
    row8 = iota((n, n), 0)
    shift = ones((iota((n, n), 1) + 1 == row8) & (lax.rem(row8, 2) == 1))
    skip = dot(shift, mine.astype(BF16))
    pair_rank = rank_row + jnp.sum(
        hot_row * skip[:, 0:1], axis=0, keepdims=True
    ).astype(jnp.int32)
    pair_row = lax.shift_right_logical(ids_row, 1)

    def own_rows(role):
        e = 2 * roles[role]
        return (counts[pl.ds(e, 1), :] + counts[pl.ds(e + 1, 1), :])[:, 0:1]

    zero1 = jnp.zeros((1, 1), jnp.int32)
    to_o = jnp.where(inner, zero1, LOCAL_KEY)
    to_i = jnp.where(inner, LOCAL_KEY, own_rows("p") + own_rows("q"))
    to_p = jnp.where(inner, zero1 + FAR_KEY, 0)
    to_q = own_rows("p") + to_p
    key = jnp.zeros((1, tok), jnp.int32)
    for role, to in (("o", to_o), ("i", to_i), ("p", to_p), ("q", to_q)):
        key = jnp.where(pair_row == roles[role], to + pair_rank, key)
    tok_key[...] = key

    def near_copy(j, slot):
        return pltpu.make_async_remote_copy(
            src_ref=outbox.at[slot, pl.ds(0, block)],
            dst_ref=inbox.at[pl.ds(pl.multiple_of(j * two, two), block)],
            send_sem=near_send.at[slot], recv_sem=near_recv.at[j],
            device_id={"expert": near_dev}, device_id_type=MESH,
        )

    def far_copy(j, slot):
        return pltpu.make_async_remote_copy(
            src_ref=outbox.at[slot, pl.ds(block, block)],
            dst_ref=inbox.at[pl.ds(pl.multiple_of(j * two + block, block), block)],
            send_sem=far_send.at[slot], recv_sem=far_recv.at[j],
            device_id={"expert": far_dev}, device_id_type=MESH,
        )

    def count(dest, source):
        return pltpu.make_async_remote_copy(
            src_ref=counts, dst_ref=count_all.at[source],
            send_sem=count_send.at[dest], recv_sem=count_recv.at[source],
            device_id={"expert": dest}, device_id_type=MESH,
        )

    def total(dest, source):
        return pltpu.make_async_remote_copy(
            src_ref=totals, dst_ref=total_all.at[source],
            send_sem=total_send.at[dest], recv_sem=total_recv.at[source],
            device_id={"dp": dest}, device_id_type=MESH,
        )

    def far_on(k):
        return inner & (k < far_blocks)

    def sent(k):
        slot = lax.rem(k, ring)

        @pl.when(k < near_limit)
        def _():
            near_copy(k, slot).wait_send()

        @pl.when(far_on(k))
        def _():
            far_copy(k, slot).wait_send()

    def pack(k, low, high):
        slot = lax.rem(k, ring)
        row = iota((two, 1), 0)
        want = jnp.where(row < block, k * block + row, FAR_KEY + k * block + row - block)
        picks = []
        if low < base:
            picks.append(ones(want == tok_key[...]))
        if high > base:
            picks.append(ones(want == in_key[:, max(low, base) - base : high - base]))
        pick = picks[0] if len(picks) == 1 else jnp.concatenate(picks, axis=1)
        for at in range(0, width, piece):
            outbox[slot, :, at : at + piece] = dot(
                pick, pool[low:high, at : at + piece]
            ).astype(BF16)

    def launch(k):
        slot = lax.rem(k, ring)

        @pl.when(k < near_limit)
        def _():
            near_copy(k, slot).start()

        @pl.when(far_on(k))
        def _():
            far_copy(k, slot).start()

    def arrive(b):
        at = pl.multiple_of(b * two, two)
        near_copy(b, 0).wait_recv()
        pool[pl.ds(base + at, block), :] = inbox[pl.ds(at, block), :]

        @pl.when(far_on(b))
        def _():
            far_copy(b, 0).wait_recv()
            pool[pl.ds(base + at + block, block), :] = inbox[pl.ds(at + block, block), :]

    def ffn(rows, code):
        parts = []
        wide = jnp.broadcast_to(code, (pair, hidden))
        for parity in (0, 1):
            gate = dot(rows, gate_ref[parity])
            up = dot(rows, up_ref[parity])
            act = gate / (1.0 + jnp.exp(-gate)) * up
            parts.append(jnp.where(wide == parity + 1, act, 0.0).astype(BF16))
        act = jnp.concatenate(parts, axis=1)
        return [
            dot(act, down_ref[:, at : at + piece]) for at in range(0, width, piece)
        ]

    load_tok.wait()
    pack(0, tok_at, base)
    pl.semaphore_wait(barrier, n + dps - 2)
    launch(0)

    def tell(i, c):
        count(lax.rem(me + i, n), me).start()
        return c

    lax.fori_loop(1, n, tell, 0)
    for copy in share:
        copy.start()
    for k in range(1, LAG):
        pack(k, tok_at, base)
        launch(k)
    count_all[me] = counts[...]

    spare = pool.at[pl.ds(base, blocks * two)]

    def clear(i, c):
        spare[pl.ds(pl.multiple_of(i * two, two), two), :] = jnp.zeros((two, width), BF16)
        return c

    lax.fori_loop(0, blocks, clear, 0)

    def heard(i, c):
        count(me, lax.rem(me + i, n)).wait_recv()
        return c

    lax.fori_loop(1, n, heard, 0)

    def rows_of(lane):
        def get(h, a, b):
            a, b = (FLIP[a], FLIP[b]) if h else (a, b)
            dev, e = 2 * roles[a] + lane, 2 * roles[b]
            return count_all[dev, pl.ds(e, 1), :] + count_all[dev, pl.ds(e + 1, 1), :]

        return get

    def even(a):
        return count_all[2 * roles[a] + core, pl.ds(2 * chip, 1), :][:, 0:1]

    place, ends = lay_streams(rows_of(core), block)
    over = jnp.zeros((1, LANES), jnp.int32)
    for lane_place, lane_ends in (
        (place, ends), lay_streams(rows_of(1 - core), block)
    ):
        for (s, _), end in lane_ends.items():
            limit = {"A": near_blocks - LAG, "M": far_blocks, "B": near_blocks}[s] * block
            over = jnp.maximum(over, (end > limit).astype(jnp.int32))
        for name, (first, size) in lane_place.items():
            if name[2] == "go":
                bad = (first + size > go_blocks * block) & (size > 0)
            else:
                bad = (first < back_blocks * block) & (size > 0)
            over = jnp.maximum(over, bad.astype(jnp.int32))

    def at(name):
        first, size = place[name]
        return first[:, 0:1], size[:, 0:1]

    def choose(a, b):
        return tuple(jnp.where(inner, x, y) for x, y in zip(at(a), at(b)))

    def start(name):
        return at(name)[0]

    lane = iota((1, blocks * two), 1)
    inside = lax.rem(lane, two)
    is_far = inside >= block
    spot = lax.div(lane, two) * block + lax.rem(inside, block)
    nowhere = zero1 - 65536
    code = jnp.full((1, blocks * two), -1, jnp.int32)
    near_runs = (
        (("A", 0, "go", "o", "p"), ("B", 0, "go", "i", "o"),
         FAR_KEY + start(("M", 0, "go", "o", "p")), start(("A", 0, "ret", "o", "i"))),
        (("A", 0, "go", "o", "q"), ("B", 0, "go", "p", "o"),
         FAR_KEY + start(("M", 0, "go", "o", "q")), start(("A", 0, "ret", "o", "p"))),
        (("A", 0, "go", "o", "i"), ("B", 0, "go", "q", "o"),
         start(("B", 0, "ret", "i", "o")), start(("A", 0, "ret", "o", "q"))),
        (("A", 0, "ret", "o", "p"), ("B", 0, "ret", "p", "o"),
         FAR_KEY + start(("M", 0, "ret", "o", "p")), nowhere),
        (("A", 0, "ret", "o", "q"), ("B", 0, "ret", "q", "o"),
         FAR_KEY + start(("M", 0, "ret", "o", "q")), nowhere),
    )
    for in_run, out_run, to_in, to_out in near_runs:
        first, size = choose(in_run, out_run)
        to = jnp.where(inner, to_in, to_out)
        hit = (spot >= first) & (spot < first + size) & jnp.logical_not(is_far)
        code = jnp.where(hit, spot + (to - first), code)
    far_runs = (
        (("M", 1, "go", "i", "p"), FAR_KEY + start(("M", 0, "ret", "i", "p"))),
        (("M", 1, "go", "i", "q"), start(("B", 0, "go", "p", "o"))),
        (("M", 1, "go", "o", "p"), FAR_KEY + start(("M", 0, "ret", "i", "q"))),
        (("M", 1, "go", "o", "q"), start(("B", 0, "go", "q", "o"))),
        (("M", 1, "ret", "i", "q"), start(("B", 0, "ret", "p", "o"))),
        (("M", 1, "ret", "o", "q"), start(("B", 0, "ret", "q", "o"))),
    )
    for run, to in far_runs:
        first, size = at(run)
        hit = (spot >= first) & (spot < first + size) & is_far
        code = jnp.where(hit, spot + (to - first), code)
    in_key[...] = code

    mine_runs = []
    for in_run, out_run, far_side, a_in, a_out in (
        (("A", 0, "go", "o", "i"), ("B", 0, "go", "i", "o"), 0, "o", "i"),
        (("M", 1, "go", "i", "p"), ("B", 0, "go", "p", "o"), 1, "p", "p"),
        (("M", 1, "go", "o", "p"), ("B", 0, "go", "q", "o"), 1, "q", "q"),
    ):
        first, size = choose(in_run, out_run)
        split = jnp.where(inner, even(a_in), even(a_out))
        mine_runs.append((first, size, split, far_side * is_inner))

    mine_pairs = go_blocks // 2

    def mark(m):
        row = iota((pair, 1), 0)
        side = lax.div(lax.rem(row, two), block)
        spot = (2 * m + lax.div(row, two)) * block + lax.rem(row, block)
        code = jnp.zeros((pair, 1), jnp.int32)
        for first, size, split, which in mine_runs:
            hit = (spot >= first) & (spot < first + size) & (side == which)
            code = jnp.where(hit, jnp.where(spot - first >= split, 2, 1), code)
        rank = (m - mine_pairs) * pair + row
        first = counts[pl.ds(2 * chip, 1), :][:, 0:1]
        both = first + counts[pl.ds(2 * chip + 1, 1), :][:, 0:1]
        local = jnp.where(rank < both, jnp.where(rank >= first, 2, 1), 0)
        return jnp.where(m < mine_pairs, code, local)

    home = zero1

    def pool_at(run, side):
        def get(rank):
            spot = start(run) + rank
            return (
                base + lax.div(spot, block) * two + lax.rem(spot, block) + side * block
            )

        return get

    back_in = {
        "o": pool_at(("A", 0, "ret", "o", "i"), 0),
        "p": pool_at(("M", 1, "ret", "i", "p"), 1),
        "q": pool_at(("M", 1, "ret", "o", "p"), 1),
        "i": lambda rank: home + rank,
    }
    back_out = {
        "i": pool_at(("B", 0, "ret", "i", "o"), 0),
        "p": pool_at(("B", 0, "ret", "p", "o"), 0),
        "q": pool_at(("B", 0, "ret", "q", "o"), 0),
        "o": lambda rank: home + rank,
    }
    from_row = jnp.zeros((1, tok), jnp.int32)
    for role in "oipq":
        found = jnp.where(inner, back_in[role](pair_rank), back_out[role](pair_rank))
        from_row = jnp.where(pair_row == roles[role], found, from_row)

    def add(i, carry):
        before, whole = carry
        here = count_all[i]
        return before + here * (i < me).astype(jnp.int32), whole + here

    zero = jnp.zeros((n, LANES), jnp.int32)
    before, whole = lax.fori_loop(0, n, add, (zero, zero))
    over = jnp.broadcast_to(over, (n, LANES))
    totals[0] = whole
    totals[1] = over
    total_all[group, 0] = whole
    total_all[group, 1] = over

    def tell_dp(i, c):
        total(lax.rem(group + i, dps), group).start()
        return c

    lax.fori_loop(1, dps, tell_dp, 0)

    def work(m):
        at = jnp.where(m < mine_pairs, base + m * pair, (m - mine_pairs) * pair)
        at = pl.multiple_of(at, pair)
        code = mark(m)
        done = ffn(pool[pl.ds(at, pair), :], code)
        wide = jnp.broadcast_to(code, (pair, piece))
        for i, part in enumerate(done):
            cols = slice(i * piece, (i + 1) * piece)
            raw = pool[pl.ds(at, pair), cols].astype(F32)
            pool[pl.ds(at, pair), cols] = jnp.where(wide > 0, part, raw).astype(BF16)

    own_end = tok // block
    cuts = [LAG, LAG + 4, LAG + 8, own_end]
    while cuts[-1] < steps:
        ahead = (cuts[-1] - LAG) // 4 * 4 + 4 + LAG
        cuts.append(min(steps, ahead))

    def step(busy, first, last):
        def run(k, c):
            arrive(k - LAG)

            @pl.when(k >= ring)
            def _():
                sent(k - ring)

            for lo, hi in zip(cuts[:-1], cuts[1:]):
                if hi <= first or lo >= last:
                    continue

                @pl.when((k >= lo) & (k < hi) & (k < near_limit))
                def _():
                    pack(
                        k, tok_at if lo < own_end else base, base + (hi - LAG) * two
                    )

            launch(k)
            if busy:
                m = jnp.where(k < switch, k - HOLD, lax.div(k - LAG - 1, 2))

                @pl.when(
                    ((k < switch) | (lax.rem(k - LAG, 2) == 1)) & (m < mine_pairs + 2)
                )
                def _():
                    work(m)

            return c

        lax.fori_loop(first, last, run, 0)

    switch = 2 * HOLD - LAG
    step(False, LAG, HOLD)

    def gather_local(i, c):
        rank = i * pair + iota((pair, 1), 0)
        at = pl.multiple_of(i * pair, pair)
        pick = ones(rank + LOCAL_KEY == tok_key[...])
        for col in range(0, width, piece):
            pool[pl.ds(at, pair), col : col + piece] = dot(
                pick, pool[tok_at:base, col : col + piece]
            ).astype(BF16)
        return c

    lax.fori_loop(0, 2, gather_local, 0)

    for copy in own:
        copy.wait()
    for copy in arriving:
        copy.wait_recv()
    step(True, HOLD, steps)

    def heard_dp(i, c):
        total(group, lax.rem(group + i, dps)).wait_recv()
        return c

    lax.fori_loop(1, dps, heard_dp, 0)

    def add_dp(i, carry):
        outer, most = carry
        return (
            outer + total_all[i, 0] * (i < group).astype(jnp.int32),
            jnp.maximum(most, total_all[i, 1]),
        )

    outer, most = lax.fori_loop(0, dps, add_dp, (zero, over))
    offset = before + outer
    flag_ref[...] = most[0:1, 0:1]
    slot = jnp.sum(
        hot_row * offset[:, 0:1].astype(F32), axis=0, keepdims=True
    ).astype(jnp.int32) + rank_row
    slot_ref[...] = slot
    from_row = jnp.where(slot < capacity, from_row, -1)
    position[...] = jnp.transpose(
        jnp.broadcast_to(from_row, (8, tok)).astype(F32)
    )[:, 0:1].astype(jnp.int32)

    span = 8 * two

    def combine(at, size, first):
        pick = ones(position[...] == iota((1, size), 1) + at)
        rows = pl.ds(at if isinstance(at, int) else pl.multiple_of(at, two), size)
        for col in range(0, width, piece):
            part = dot(pick, pool[rows, col : col + piece]).astype(BF16)
            if first:
                out_ref[:, col : col + piece] = part
            else:
                out_ref[:, col : col + piece] += part

    combine(0, tok_at, True)
    seen = base + (steps - LAG) * two
    whole_at = base + back_blocks * two
    spans = (seen - whole_at) // span

    def combine_step(c, carry):
        combine(whole_at + c * span, span, False)
        return carry

    lax.fori_loop(0, spans, combine_step, 0)
    if whole_at + spans * span < seen:
        combine(whole_at + spans * span, seen - whole_at - spans * span, False)

    def late(b, c):
        arrive(b)
        return c

    lax.fori_loop(steps - LAG, near_blocks - LAG * is_inner, late, 0)
    combine(seen, pool.shape[0] - seen, False)

    def flush(k, c):
        sent(k)
        return c

    lax.fori_loop(steps - ring, steps, flush, 0)
    for copy in share:
        copy.wait_send()

    def drain(i, c):
        count(lax.rem(me + i, n), me).wait_send()
        return c

    lax.fori_loop(1, n, drain, 0)

    def drain_dp(i, c):
        total(lax.rem(group + i, dps), group).wait_send()
        return c

    lax.fori_loop(1, dps, drain_dp, 0)


def streamed(tokens, expert_ids, gate_proj, up_proj, down_proj):
    tok, width = tokens.shape
    hidden = gate_proj.shape[2]
    n = lax.axis_size("expert")
    dps = lax.axis_size("dp")
    capacity = tok * dps
    block = tok // (2 * n)
    far_blocks = 9 * n // 2
    near_blocks = far_blocks + LAG
    go_blocks = 13 * n // 4
    back_blocks = n
    blocks = near_blocks
    ring = 4
    vmem = pl.BlockSpec(memory_space=pltpu.VMEM)
    anywhere = pl.BlockSpec(memory_space=pltpu.MemorySpace.HBM)
    dma = pltpu.SemaphoreType.DMA
    table = pltpu.VMEM((n, LANES), jnp.int32)
    mixed, slot, flag = pl.pallas_call(
        functools.partial(
            stream_kernel, n, dps, capacity, block, near_blocks, far_blocks, go_blocks,
            back_blocks,
        ),
        out_shape=(
            jax.ShapeDtypeStruct((tok, width), BF16),
            jax.ShapeDtypeStruct((1, tok), jnp.int32),
            jax.ShapeDtypeStruct((1, 1), jnp.int32),
        ),
        in_specs=[vmem, anywhere, anywhere, anywhere, anywhere],
        out_specs=(vmem, vmem, vmem),
        scratch_shapes=[
            pltpu.VMEM((2, width, hidden), BF16),
            pltpu.VMEM((2, width, hidden), BF16),
            pltpu.VMEM((2 * hidden, width), BF16),
            pltpu.VMEM((8 * block + tok + 2 * block * blocks, width), BF16),
            pltpu.VMEM((2 * block * blocks, width), BF16),
            pltpu.VMEM((ring, 2 * block, width), BF16),
            pltpu.VMEM((1, tok), jnp.int32),
            pltpu.VMEM((1, 2 * block * blocks), jnp.int32),
            pltpu.VMEM((tok, 1), jnp.int32),
            table,
            pltpu.VMEM((n, n, LANES), jnp.int32),
            pltpu.VMEM((2, n, LANES), jnp.int32),
            pltpu.VMEM((dps, 2, n, LANES), jnp.int32),
            dma((1,)), dma((3,)), dma((3,)), dma((3,)),
            dma((ring,)), dma((near_blocks,)), dma((ring,)), dma((far_blocks,)),
            dma((n,)), dma((n,)), dma((dps,)), dma((dps,)),
        ],
        compiler_params=pltpu.CompilerParams(
            collective_id=0, has_side_effects=True, vmem_limit_bytes=60 * 2**20
        ),
    )(expert_ids.reshape(1, tok), tokens, gate_proj, up_proj, down_proj)
    return lax.cond(
        flag[0, 0] > 0,
        lambda: padded(tokens, expert_ids, gate_proj, up_proj, down_proj),
        lambda: (mixed, slot.reshape(tok)),
    )


def on_device(tokens, expert_ids, gate_proj, up_proj, down_proj):
    n = lax.axis_size("expert")
    if n == 8 and tokens.shape[0] // n % 64 == 0:
        return streamed(tokens, expert_ids, gate_proj, up_proj, down_proj)
    return direct(tokens, expert_ids, gate_proj, up_proj, down_proj)


def solution(mesh):
    in_specs = (
        P(("dp", "expert"), None),
        P(("dp", "expert"), None),
        P("expert", None, None),
        P("expert", None, None),
        P("expert", None, None),
    )
    out_specs = (P(("dp", "expert"), None), P(("dp", "expert")))
    return jax.shard_map(
        on_device, mesh=mesh, in_specs=in_specs, out_specs=out_specs, check_vma=False
    )
```

```python
import functools

import jax
import jax.numpy as jnp
from jax import lax
from jax.experimental import pallas as pl
from jax.experimental.pallas import tpu as pltpu
from jax.sharding import PartitionSpec as P

MESH = pl.DeviceIdType.MESH
F32 = jnp.float32
BF16 = jnp.bfloat16
LANES = 128
LAG, HOLD, REST = 3, 7, 23


def spread(step, n):
    half = (step // 2) * (2 * (step % 2) - 1)
    return jnp.where(step == 0, 0, n // 2 + half)


def direct_kernel(
    n, dps, most, capacity,
    row_ids, col_ids, tok_ref, gate_hbm, up_hbm, down_hbm,
    out_ref, slot_ref,
    gate_ref, up_ref, down_ref, outgoing, arrived, results, returned,
    position, offset, counts, count_all, totals, total_all,
    weight_sem, go_send, go_recv, back_send, back_recv,
    count_send, count_recv, total_send, total_recv,
):
    me = lax.axis_index("expert")
    group = lax.axis_index("dp")
    tok = tok_ref.shape[0]
    width = tok_ref.shape[1]

    weights = [
        pltpu.make_async_copy(src.at[0], dst, weight_sem.at[i])
        for i, (src, dst) in enumerate(
            ((gate_hbm, gate_ref), (up_hbm, up_ref), (down_hbm, down_ref))
        )
    ]
    for copy in weights:
        copy.start()

    barrier = pltpu.get_barrier_semaphore()

    def greet(i, c):
        pl.semaphore_signal(
            barrier, inc=1, device_id={"expert": lax.rem(me + i, n)}, device_id_type=MESH
        )
        return c

    def greet_dp(i, c):
        pl.semaphore_signal(
            barrier, inc=1, device_id={"dp": lax.rem(group + i, dps)}, device_id_type=MESH
        )
        return c

    lax.fori_loop(1, n, greet, 0)
    lax.fori_loop(1, dps, greet_dp, 0)

    earlier = lax.broadcasted_iota(jnp.int32, (tok, tok), 0) < lax.broadcasted_iota(
        jnp.int32, (tok, tok), 1
    )
    later = lax.broadcasted_iota(jnp.int32, (tok, tok), 0) > lax.broadcasted_iota(
        jnp.int32, (tok, tok), 1
    )
    ids_row = row_ids[...]
    hot_row = (ids_row == lax.broadcasted_iota(jnp.int32, (n, tok), 0)).astype(F32)
    before_row = jnp.dot(
        hot_row.astype(BF16), earlier.astype(F32).astype(BF16), preferred_element_type=F32
    )
    rank_row = jnp.sum(before_row * hot_row, axis=0, keepdims=True).astype(jnp.int32)
    pos_row = ids_row * most + rank_row
    counts[...] = jnp.broadcast_to(
        jnp.sum(hot_row, axis=1, keepdims=True), (n, LANES)
    ).astype(jnp.int32)

    ids_col = col_ids[...]
    hot_col = (ids_col == lax.broadcasted_iota(jnp.int32, (tok, n), 1)).astype(F32)
    before_col = jnp.dot(
        later.astype(F32).astype(BF16), hot_col.astype(BF16), preferred_element_type=F32
    )
    rank_col = jnp.sum(before_col * hot_col, axis=1, keepdims=True).astype(jnp.int32)
    position[...] = ids_col * most + rank_col

    def go(dest, source):
        return pltpu.make_async_remote_copy(
            src_ref=outgoing.at[dest], dst_ref=arrived.at[source],
            send_sem=go_send.at[dest], recv_sem=go_recv.at[source],
            device_id={"expert": dest}, device_id_type=MESH,
        )

    def back(dest, source):
        return pltpu.make_async_remote_copy(
            src_ref=results.at[dest], dst_ref=returned.at[source],
            send_sem=back_send.at[dest], recv_sem=back_recv.at[source],
            device_id={"expert": dest}, device_id_type=MESH,
        )

    def count(dest, source):
        return pltpu.make_async_remote_copy(
            src_ref=counts, dst_ref=count_all.at[source],
            send_sem=count_send.at[dest], recv_sem=count_recv.at[source],
            device_id={"expert": dest}, device_id_type=MESH,
        )

    def total(dest, source):
        return pltpu.make_async_remote_copy(
            src_ref=totals, dst_ref=total_all.at[source],
            send_sem=total_send.at[dest], recv_sem=total_recv.at[source],
            device_id={"dp": dest}, device_id_type=MESH,
        )

    def pack(dest):
        pick = (
            lax.broadcasted_iota(jnp.int32, (most, tok), 0) + dest * most == pos_row
        ).astype(F32).astype(BF16)
        return jnp.dot(pick, tok_ref[...], preferred_element_type=F32).astype(BF16)

    pl.semaphore_wait(barrier, n + dps - 2)

    def dispatch(i, c):
        dest = lax.rem(me + spread(i, n), n)
        outgoing[dest] = pack(dest)
        go(dest, me).start()
        return c

    lax.fori_loop(1, n, dispatch, 0)

    def tell(i, c):
        count(lax.rem(me + i, n), me).start()
        return c

    lax.fori_loop(1, n, tell, 0)
    count_all[me] = counts[...]
    arrived[me] = pack(me)

    for copy in weights:
        copy.wait()

    def ffn(source):
        rows = arrived[source]
        gate = jnp.dot(rows, gate_ref[...], preferred_element_type=F32)
        up = jnp.dot(rows, up_ref[...], preferred_element_type=F32)
        hidden = (gate / (1.0 + jnp.exp(-gate)) * up).astype(BF16)
        return jnp.dot(hidden, down_ref[...], preferred_element_type=F32).astype(BF16)

    def expert_step(i, c):
        source = lax.rem(me + n - spread(i, n), n)

        @pl.when(i > 0)
        def _():
            go(me, source).wait_recv()

        results[source] = ffn(source)

        @pl.when(i > 0)
        def _():
            back(source, me).start()

        return c

    lax.fori_loop(0, n, expert_step, 0)

    def heard(i, c):
        count(me, lax.rem(me + i, n)).wait_recv()
        return c

    lax.fori_loop(1, n, heard, 0)

    def add(i, carry):
        inner, whole = carry
        here = count_all[i]
        return inner + here * (i < me).astype(jnp.int32), whole + here

    zero = jnp.zeros((n, LANES), jnp.int32)
    inner, whole = lax.fori_loop(0, n, add, (zero, zero))
    totals[...] = whole

    def tell_dp(i, c):
        total(lax.rem(group + i, dps), group).start()
        return c

    lax.fori_loop(1, dps, tell_dp, 0)
    total_all[group] = whole

    def heard_dp(i, c):
        total(group, lax.rem(group + i, dps)).wait_recv()
        return c

    lax.fori_loop(1, dps, heard_dp, 0)

    def add_dp(i, outer):
        return outer + total_all[i] * (i < group).astype(jnp.int32)

    offset[...] = inner + lax.fori_loop(0, dps, add_dp, zero)
    slot_ref[...] = (
        jnp.sum(
            hot_row * offset[:, 0:1].astype(F32), axis=0, keepdims=True
        ).astype(jnp.int32)
        + rank_row
    )

    piece = min(width, 512)

    def combine(source, block, first):
        lane = lax.broadcasted_iota(jnp.int32, (tok, most), 1)
        fits = offset[pl.ds(source, 1), 0:most] + lax.broadcasted_iota(
            jnp.int32, (1, most), 1
        ) < capacity
        pick = (lane + source * most == position[...]) & fits
        pick = pick.astype(F32).astype(BF16)
        for at in range(0, width, piece):
            part = jnp.dot(
                pick, block[source, :, at : at + piece], preferred_element_type=F32
            ).astype(BF16)
            if first:
                out_ref[:, at : at + piece] = part
            else:
                out_ref[:, at : at + piece] += part

    combine(me, results, True)

    def combine_step(i, c):
        source = lax.rem(me + n - spread(i, n), n)
        back(me, source).wait_recv()
        combine(source, returned, False)
        return c

    lax.fori_loop(1, n, combine_step, 0)

    def drain(i, c):
        other = lax.rem(me + i, n)
        go(other, me).wait_send()
        back(other, me).wait_send()
        count(other, me).wait_send()
        return c

    lax.fori_loop(1, n, drain, 0)

    def drain_dp(i, c):
        total(lax.rem(group + i, dps), group).wait_send()
        return c

    lax.fori_loop(1, dps, drain_dp, 0)


def direct(tokens, expert_ids, gate_proj, up_proj, down_proj):
    tok, width = tokens.shape
    hidden = gate_proj.shape[2]
    n = lax.axis_size("expert")
    dps = lax.axis_size("dp")
    most = 2 * tok // n
    capacity = tok * dps
    vmem = pl.BlockSpec(memory_space=pltpu.VMEM)
    anywhere = pl.BlockSpec(memory_space=pltpu.MemorySpace.HBM)
    dma = pltpu.SemaphoreType.DMA
    block = pltpu.VMEM((n, most, width), BF16)
    mixed, slot = pl.pallas_call(
        functools.partial(direct_kernel, n, dps, most, capacity),
        out_shape=(
            jax.ShapeDtypeStruct((tok, width), BF16),
            jax.ShapeDtypeStruct((1, tok), jnp.int32),
        ),
        in_specs=[vmem, vmem, vmem, anywhere, anywhere, anywhere],
        out_specs=(vmem, vmem),
        scratch_shapes=[
            pltpu.VMEM((width, hidden), BF16),
            pltpu.VMEM((width, hidden), BF16),
            pltpu.VMEM((hidden, width), BF16),
            block, block, block, block,
            pltpu.VMEM((tok, 1), jnp.int32),
            pltpu.VMEM((n, LANES), jnp.int32),
            pltpu.VMEM((n, LANES), jnp.int32),
            pltpu.VMEM((n, n, LANES), jnp.int32),
            pltpu.VMEM((n, LANES), jnp.int32),
            pltpu.VMEM((dps, n, LANES), jnp.int32),
            dma((3,)), dma((n,)), dma((n,)), dma((n,)), dma((n,)),
            dma((n,)), dma((n,)), dma((dps,)), dma((dps,)),
        ],
        compiler_params=pltpu.CompilerParams(
            collective_id=0, has_side_effects=True, vmem_limit_bytes=60 * 2**20
        ),
    )(
        expert_ids.reshape(1, tok), expert_ids, tokens, gate_proj, up_proj, down_proj
    )
    return mixed, slot.reshape(tok)


def entering(part, axis, combine, identity):
    place = lax.axis_index(axis)
    gathered = lax.all_gather(part, axis)
    state = jnp.zeros_like(part) + jnp.asarray(identity, part.dtype)

    def one(hop, state):
        return combine(state, lax.dynamic_index_in_dim(gathered, hop, 0, False))

    return lax.fori_loop(0, place, one, state)


def add_counts(earlier, later):
    return earlier + later


def expert_ffn(rows, gate_proj, up_proj, down_proj):
    gate_val = jnp.dot(rows, gate_proj[0], preferred_element_type=jnp.float32)
    up_val = jnp.dot(rows, up_proj[0], preferred_element_type=jnp.float32)
    hidden = (jax.nn.silu(gate_val) * up_val).astype(jnp.bfloat16)
    return jnp.dot(hidden, down_proj[0], preferred_element_type=jnp.float32).astype(jnp.bfloat16)


def padded(tokens, expert_ids, gate_proj, up_proj, down_proj):
    tok_rows, width = tokens.shape
    experts_all = lax.axis_size("expert")
    most = 2 * tok_rows // experts_all
    capacity = tok_rows * lax.axis_size("dp")
    choices = expert_ids[:, 0]
    onehot = (choices[:, None] == jnp.arange(experts_all, dtype=jnp.int32)[None, :]).astype(
        jnp.int32
    )
    counts = jnp.sum(onehot, axis=0)
    inner = entering(counts, "expert", add_counts, jnp.zeros_like(counts))
    totals = lax.psum(counts, "expert")
    outer = entering(totals, "dp", add_counts, jnp.zeros_like(totals))
    offset = inner + outer
    before = jnp.cumsum(onehot, axis=0) - onehot
    local_rank = jnp.sum(before * onehot, axis=1)
    global_slot = (jnp.sum(onehot * offset[None, :], axis=1) + local_rank).astype(jnp.int32)
    is_kept = global_slot < capacity
    position = choices * most + local_rank
    targets = jnp.arange(experts_all * most, dtype=jnp.int32)
    dispatch = ((targets[:, None] == position[None, :]) & is_kept[None, :]).astype(jnp.bfloat16)
    outgoing = jnp.dot(dispatch, tokens, preferred_element_type=jnp.float32).astype(jnp.bfloat16)
    outgoing = outgoing.reshape(experts_all, most, width)
    arrived = lax.all_to_all(outgoing, "expert", split_axis=0, concat_axis=0, tiled=True)
    sources, slots_here, _ = arrived.shape
    flat = arrived.reshape(sources * slots_here, width)
    returned = lax.all_to_all(
        expert_ffn(flat, gate_proj, up_proj, down_proj).reshape(sources, slots_here, width),
        "expert",
        split_axis=0,
        concat_axis=0,
        tiled=True,
    )
    flat_back = returned.reshape(experts_all * most, width)
    mixed = lax.dot_general(
        dispatch, flat_back, (((0,), (0,)), ((), ())), preferred_element_type=jnp.float32
    )
    return (mixed.astype(jnp.bfloat16), global_slot)


RUN_ORDER = {
    "A": ("go op", "go oq", "go oi", "ret op", "ret oq", "ret oi"),
    "M": (
        "go ip", "go iq", "go oq", "go op", "ret ip", "ret op", "ret iq", "ret oq",
    ),
    "B": ("go io", "go po", "go qo", "ret io", "ret po", "ret qo"),
}
FLIP = {"o": "q", "i": "p", "p": "i", "q": "o"}
FAR_KEY = 4096
LOCAL_KEY = 8192


def lay_streams(rows_of, block):
    place, end = {}, {}
    queue = {
        (s, h): [(run[:-3], run[-2], run[-1]) for run in RUN_ORDER[s]]
        for s in "AMB" for h in (0, 1)
    }
    zero = jnp.zeros((1, LANES), jnp.int32)
    for name in queue:
        end[name] = zero
    while any(queue.values()):
        for (s, h), runs in queue.items():
            while runs:
                kind, a, b = runs[0]
                fa, fb = FLIP[a], FLIP[b]
                need, result = None, kind == "ret"
                if s == "A" and kind == "ret":
                    need = ("B", h, "go", b, a)
                elif s == "M" and a == "o":
                    need, result = ("A", h, kind, a, b), False
                elif s == "M" and kind == "ret":
                    need = ("M", 1 - h, "go", fb, fa)
                elif s == "B" and a != "i":
                    need, result = ("M", 1 - h, kind, fa, fb), False
                elif s == "B" and kind == "ret":
                    need = ("A", h, "go", b, a)
                if need is not None and need not in place:
                    break
                size = rows_of(h, a, b) if kind == "go" else rows_of(h, b, a)
                first = end[(s, h)]
                if need is not None:
                    there = place[need][0]
                    ready = there + block * LAG
                    if result:
                        ready = jnp.maximum(
                            ready + block * 2,
                            lax.shift_right_logical(there, 1) + block * (HOLD + 1),
                        )
                    if s == "B":
                        ready -= block * jnp.clip(ready // block - REST, 0, LAG)
                    first = jnp.where(size > 0, jnp.maximum(first, ready), first)
                place[(s, h, kind, a, b)] = (first, size)
                end[(s, h)] = first + size
                runs.pop(0)
    return place, end


def stream_kernel(
    n, dps, capacity, block, near_blocks, far_blocks, go_blocks, back_blocks,
    row_ids, tok_hbm, gate_hbm, up_hbm, down_hbm,
    out_ref, slot_ref, flag_ref,
    gate_ref, up_ref, down_ref, pool, inbox, outbox,
    tok_key, in_key, position, counts, count_all, totals, total_all,
    tok_sem, own_sem, pair_send, pair_recv, near_send, near_recv, far_send, far_recv,
    count_send, count_recv, total_send, total_recv,
):
    me = lax.axis_index("expert")
    group = lax.axis_index("dp")
    tok = row_ids.shape[1]
    width = pool.shape[1]
    hidden = gate_ref.shape[2]
    core = lax.rem(me, 2)
    chip = lax.div(me, 2)
    half = lax.div(chip, 2)
    roles = {"o": 3 * half, "i": 1 + half, "p": 2 - half, "q": 3 - 3 * half}
    inner = chip == roles["i"]
    is_inner = inner.astype(jnp.int32)
    near_dev = me + 2 - 4 * lax.rem(chip, 2)
    far_dev = 2 * (3 - chip) + core
    pair_dev = me + 1 - 2 * core
    two = 2 * block
    blocks = inbox.shape[0] // two
    pair = 2 * two
    steps = far_blocks + LAG
    b_blocks = far_blocks
    tok_at = 2 * pair
    base = tok_at + tok
    piece = min(width, 1024)
    ring = outbox.shape[0]

    def iota(shape, axis):
        return lax.broadcasted_iota(jnp.int32, shape, axis)

    def ones(mask):
        return mask.astype(F32).astype(BF16)

    def dot(a, b):
        return jnp.dot(a, b, preferred_element_type=F32)

    load_tok = pltpu.make_async_copy(tok_hbm, pool.at[pl.ds(tok_at, tok)], tok_sem.at[0])
    load_tok.start()
    mine_down = pl.ds(pl.multiple_of(core * hidden, hidden), hidden)
    pairs = (
        (gate_hbm, gate_ref.at[core]), (up_hbm, up_ref.at[core]),
        (down_hbm, down_ref.at[mine_down]),
    )
    own = [
        pltpu.make_async_copy(src.at[0], dst, own_sem.at[i])
        for i, (src, dst) in enumerate(pairs)
    ]
    share = [
        pltpu.make_async_remote_copy(
            src_ref=src.at[0], dst_ref=dst, send_sem=pair_send.at[i],
            recv_sem=pair_recv.at[i], device_id={"expert": pair_dev}, device_id_type=MESH,
        )
        for i, (src, dst) in enumerate(pairs)
    ]
    other_down = pl.ds(pl.multiple_of((1 - core) * hidden, hidden), hidden)
    arriving = [
        pltpu.make_async_remote_copy(
            src_ref=src.at[0], dst_ref=dst, send_sem=pair_send.at[i],
            recv_sem=pair_recv.at[i], device_id={"expert": pair_dev}, device_id_type=MESH,
        )
        for i, (src, dst) in enumerate((
            (gate_hbm, gate_ref.at[1 - core]), (up_hbm, up_ref.at[1 - core]),
            (down_hbm, down_ref.at[other_down]),
        ))
    ]
    for copy in own:
        copy.start()

    barrier = pltpu.get_barrier_semaphore()

    def greet(i, c):
        pl.semaphore_signal(
            barrier, inc=1, device_id={"expert": lax.rem(me + i, n)}, device_id_type=MESH
        )
        return c

    def greet_dp(i, c):
        pl.semaphore_signal(
            barrier, inc=1, device_id={"dp": lax.rem(group + i, dps)}, device_id_type=MESH
        )
        return c

    lax.fori_loop(1, n, greet, 0)
    lax.fori_loop(1, dps, greet_dp, 0)

    ids_row = row_ids[...]
    hot_row = (ids_row == iota((n, tok), 0)).astype(F32)
    earlier = ones(iota((LANES, LANES), 0) < iota((LANES, LANES), 1))
    ahead, mine = [], jnp.zeros((n, 1), F32)
    for lo in range(0, tok, LANES):
        hot = hot_row[:, lo : lo + LANES]
        ahead.append(dot(hot.astype(BF16), earlier) + mine)
        mine = mine + jnp.sum(hot, axis=1, keepdims=True)
    before_row = jnp.concatenate(ahead, axis=1)
    rank_row = jnp.sum(before_row * hot_row, axis=0, keepdims=True).astype(jnp.int32)
    mine = jnp.broadcast_to(mine, (n, LANES))
    counts[...] = mine.astype(jnp.int32)
    row8 = iota((n, n), 0)
    shift = ones((iota((n, n), 1) + 1 == row8) & (lax.rem(row8, 2) == 1))
    skip = dot(shift, mine.astype(BF16))
    pair_rank = rank_row + jnp.sum(
        hot_row * skip[:, 0:1], axis=0, keepdims=True
    ).astype(jnp.int32)
    pair_row = lax.shift_right_logical(ids_row, 1)

    def own_rows(role):
        e = 2 * roles[role]
        return (counts[pl.ds(e, 1), :] + counts[pl.ds(e + 1, 1), :])[:, 0:1]

    zero1 = jnp.zeros((1, 1), jnp.int32)
    to_o = jnp.where(inner, zero1, LOCAL_KEY)
    to_i = jnp.where(inner, LOCAL_KEY, own_rows("p") + own_rows("q"))
    to_p = jnp.where(inner, zero1 + FAR_KEY, 0)
    to_q = own_rows("p") + to_p
    key = jnp.zeros((1, tok), jnp.int32)
    for role, to in (("o", to_o), ("i", to_i), ("p", to_p), ("q", to_q)):
        key = jnp.where(pair_row == roles[role], to + pair_rank, key)
    tok_key[...] = key

    def near_copy(j, slot):
        return pltpu.make_async_remote_copy(
            src_ref=outbox.at[slot, pl.ds(0, block)],
            dst_ref=inbox.at[pl.ds(pl.multiple_of(j * two, two), block)],
            send_sem=near_send.at[slot], recv_sem=near_recv.at[j],
            device_id={"expert": near_dev}, device_id_type=MESH,
        )

    def far_copy(j, slot):
        return pltpu.make_async_remote_copy(
            src_ref=outbox.at[slot, pl.ds(block, block)],
            dst_ref=inbox.at[pl.ds(pl.multiple_of(j * two + block, block), block)],
            send_sem=far_send.at[slot], recv_sem=far_recv.at[j],
            device_id={"expert": far_dev}, device_id_type=MESH,
        )

    def count(dest, source):
        return pltpu.make_async_remote_copy(
            src_ref=counts, dst_ref=count_all.at[source],
            send_sem=count_send.at[dest], recv_sem=count_recv.at[source],
            device_id={"expert": dest}, device_id_type=MESH,
        )

    def total(dest, source):
        return pltpu.make_async_remote_copy(
            src_ref=totals, dst_ref=total_all.at[source],
            send_sem=total_send.at[dest], recv_sem=total_recv.at[source],
            device_id={"dp": dest}, device_id_type=MESH,
        )

    def near_at(k, rests):
        return k - rests * jnp.where(k < REST + LAG, 0, LAG)

    def near_on(k, rests):
        idle = rests * jnp.where((k >= REST) & (k < REST + LAG), 1, 0)
        return (idle == 0) & (k < near_blocks + rests * (steps - near_blocks))

    def far_on(k):
        return inner & (k < far_blocks)

    def sent(k):
        slot = lax.rem(k, ring)

        @pl.when(near_on(k, is_inner))
        def _():
            near_copy(near_at(k, is_inner), slot).wait_send()

        @pl.when(far_on(k))
        def _():
            far_copy(k, slot).wait_send()

    def pack(k, low, high):
        slot = lax.rem(k, ring)
        row = iota((two, 1), 0)
        want = jnp.where(
            row < block, near_at(k, is_inner) * block + row, FAR_KEY + k * block + row - block
        )
        picks = []
        if low < base:
            picks.append(ones(want == tok_key[...]))
        if high > base:
            picks.append(ones(want == in_key[:, max(low, base) - base : high - base]))
        pick = picks[0] if len(picks) == 1 else jnp.concatenate(picks, axis=1)
        for at in range(0, width, piece):
            outbox[slot, :, at : at + piece] = dot(
                pick, pool[low:high, at : at + piece]
            ).astype(BF16)

    def launch(k):
        slot = lax.rem(k, ring)

        @pl.when(near_on(k, is_inner))
        def _():
            near_copy(near_at(k, is_inner), slot).start()

        @pl.when(far_on(k))
        def _():
            far_copy(k, slot).start()

    def take(b):
        at = pl.multiple_of(b * two, two)
        near_copy(b, 0).wait_recv()
        pool[pl.ds(base + at, block), :] = inbox[pl.ds(at, block), :]

    def arrive(k):
        @pl.when(near_on(k, 1 - is_inner))
        def _():
            take(near_at(k, 1 - is_inner))

        @pl.when(far_on(k))
        def _():
            far_copy(k, 0).wait_recv()
            at = pl.multiple_of(k * two, two)
            pool[pl.ds(base + at + block, block), :] = inbox[pl.ds(at + block, block), :]

    def ffn(rows, code):
        parts = []
        wide = jnp.broadcast_to(code, (pair, hidden))
        for parity in (0, 1):
            gate = dot(rows, gate_ref[parity])
            up = dot(rows, up_ref[parity])
            act = gate / (1.0 + jnp.exp(-gate)) * up
            parts.append(jnp.where(wide == parity + 1, act, 0.0).astype(BF16))
        act = jnp.concatenate(parts, axis=1)
        return [
            dot(act, down_ref[:, at : at + piece]) for at in range(0, width, piece)
        ]

    load_tok.wait()
    pack(0, tok_at, base)
    pl.semaphore_wait(barrier, n + dps - 2)
    launch(0)

    def tell(i, c):
        count(lax.rem(me + i, n), me).start()
        return c

    lax.fori_loop(1, n, tell, 0)
    for copy in share:
        copy.start()
    for k in range(1, LAG):
        pack(k, tok_at, base)
        launch(k)
    count_all[me] = counts[...]

    spare = pool.at[pl.ds(base, blocks * two)]

    def clear(i, c):
        spare[pl.ds(pl.multiple_of(i * two, two), two), :] = jnp.zeros((two, width), BF16)
        return c

    lax.fori_loop(0, blocks, clear, 0)

    def heard(i, c):
        count(me, lax.rem(me + i, n)).wait_recv()
        return c

    lax.fori_loop(1, n, heard, 0)

    def rows_of(lane):
        def get(h, a, b):
            a, b = (FLIP[a], FLIP[b]) if h else (a, b)
            dev, e = 2 * roles[a] + lane, 2 * roles[b]
            return count_all[dev, pl.ds(e, 1), :] + count_all[dev, pl.ds(e + 1, 1), :]

        return get

    def even(a):
        return count_all[2 * roles[a] + core, pl.ds(2 * chip, 1), :][:, 0:1]

    place, ends = lay_streams(rows_of(core), block)
    over = jnp.zeros((1, LANES), jnp.int32)
    for lane_place, lane_ends in (
        (place, ends), lay_streams(rows_of(1 - core), block)
    ):
        for (s, _), end in lane_ends.items():
            limit = {"A": near_blocks, "M": far_blocks, "B": b_blocks}[s] * block
            over = jnp.maximum(over, (end > limit).astype(jnp.int32))
        for name, (first, size) in lane_place.items():
            if name[2] == "go":
                limit = (REST if name[0] == "B" else go_blocks) * block
                bad = (first + size > limit) & (size > 0)
            else:
                bad = (first < back_blocks * block) & (size > 0)
            over = jnp.maximum(over, bad.astype(jnp.int32))

    def at(name):
        first, size = place[name]
        return first[:, 0:1], size[:, 0:1]

    def choose(a, b):
        return tuple(jnp.where(inner, x, y) for x, y in zip(at(a), at(b)))

    def start(name):
        return at(name)[0]

    lane = iota((1, blocks * two), 1)
    inside = lax.rem(lane, two)
    is_far = inside >= block
    spot = lax.div(lane, two) * block + lax.rem(inside, block)
    nowhere = zero1 - 65536
    code = jnp.full((1, blocks * two), -1, jnp.int32)
    near_runs = (
        (("A", 0, "go", "o", "p"), ("B", 0, "go", "i", "o"),
         FAR_KEY + start(("M", 0, "go", "o", "p")), start(("A", 0, "ret", "o", "i"))),
        (("A", 0, "go", "o", "q"), ("B", 0, "go", "p", "o"),
         FAR_KEY + start(("M", 0, "go", "o", "q")), start(("A", 0, "ret", "o", "p"))),
        (("A", 0, "go", "o", "i"), ("B", 0, "go", "q", "o"),
         start(("B", 0, "ret", "i", "o")), start(("A", 0, "ret", "o", "q"))),
        (("A", 0, "ret", "o", "p"), ("B", 0, "ret", "p", "o"),
         FAR_KEY + start(("M", 0, "ret", "o", "p")), nowhere),
        (("A", 0, "ret", "o", "q"), ("B", 0, "ret", "q", "o"),
         FAR_KEY + start(("M", 0, "ret", "o", "q")), nowhere),
    )
    for in_run, out_run, to_in, to_out in near_runs:
        first, size = choose(in_run, out_run)
        to = jnp.where(inner, to_in, to_out)
        hit = (spot >= first) & (spot < first + size) & jnp.logical_not(is_far)
        code = jnp.where(hit, spot + (to - first), code)
    far_runs = (
        (("M", 1, "go", "i", "p"), FAR_KEY + start(("M", 0, "ret", "i", "p"))),
        (("M", 1, "go", "i", "q"), start(("B", 0, "go", "p", "o"))),
        (("M", 1, "go", "o", "p"), FAR_KEY + start(("M", 0, "ret", "i", "q"))),
        (("M", 1, "go", "o", "q"), start(("B", 0, "go", "q", "o"))),
        (("M", 1, "ret", "i", "q"), start(("B", 0, "ret", "p", "o"))),
        (("M", 1, "ret", "o", "q"), start(("B", 0, "ret", "q", "o"))),
    )
    for run, to in far_runs:
        first, size = at(run)
        hit = (spot >= first) & (spot < first + size) & is_far
        code = jnp.where(hit, spot + (to - first), code)
    in_key[...] = code

    mine_runs = []
    for in_run, out_run, far_side, a_in, a_out in (
        (("A", 0, "go", "o", "i"), ("B", 0, "go", "i", "o"), 0, "o", "i"),
        (("M", 1, "go", "i", "p"), ("B", 0, "go", "p", "o"), 1, "p", "p"),
        (("M", 1, "go", "o", "p"), ("B", 0, "go", "q", "o"), 1, "q", "q"),
    ):
        first, size = choose(in_run, out_run)
        split = jnp.where(inner, even(a_in), even(a_out))
        mine_runs.append((first, size, split, far_side * is_inner))

    mine_pairs = go_blocks // 2

    def mark(m):
        row = iota((pair, 1), 0)
        side = lax.div(lax.rem(row, two), block)
        spot = (2 * m + lax.div(row, two)) * block + lax.rem(row, block)
        code = jnp.zeros((pair, 1), jnp.int32)
        for first, size, split, which in mine_runs:
            hit = (spot >= first) & (spot < first + size) & (side == which)
            code = jnp.where(hit, jnp.where(spot - first >= split, 2, 1), code)
        rank = (m - mine_pairs) * pair + row
        first = counts[pl.ds(2 * chip, 1), :][:, 0:1]
        both = first + counts[pl.ds(2 * chip + 1, 1), :][:, 0:1]
        local = jnp.where(rank < both, jnp.where(rank >= first, 2, 1), 0)
        return jnp.where(m < mine_pairs, code, local)

    home = zero1

    def pool_at(run, side):
        def get(rank):
            spot = start(run) + rank
            return (
                base + lax.div(spot, block) * two + lax.rem(spot, block) + side * block
            )

        return get

    back_in = {
        "o": pool_at(("A", 0, "ret", "o", "i"), 0),
        "p": pool_at(("M", 1, "ret", "i", "p"), 1),
        "q": pool_at(("M", 1, "ret", "o", "p"), 1),
        "i": lambda rank: home + rank,
    }
    back_out = {
        "i": pool_at(("B", 0, "ret", "i", "o"), 0),
        "p": pool_at(("B", 0, "ret", "p", "o"), 0),
        "q": pool_at(("B", 0, "ret", "q", "o"), 0),
        "o": lambda rank: home + rank,
    }
    from_row = jnp.zeros((1, tok), jnp.int32)
    for role in "oipq":
        found = jnp.where(inner, back_in[role](pair_rank), back_out[role](pair_rank))
        from_row = jnp.where(pair_row == roles[role], found, from_row)

    def add(i, carry):
        before, whole = carry
        here = count_all[i]
        return before + here * (i < me).astype(jnp.int32), whole + here

    zero = jnp.zeros((n, LANES), jnp.int32)
    before, whole = lax.fori_loop(0, n, add, (zero, zero))
    over = jnp.broadcast_to(over, (n, LANES))
    totals[0] = whole
    totals[1] = over
    total_all[group, 0] = whole
    total_all[group, 1] = over

    def tell_dp(i, c):
        total(lax.rem(group + i, dps), group).start()
        return c

    lax.fori_loop(1, dps, tell_dp, 0)

    def work(m):
        at = jnp.where(m < mine_pairs, base + m * pair, (m - mine_pairs) * pair)
        at = pl.multiple_of(at, pair)
        code = mark(m)
        done = ffn(pool[pl.ds(at, pair), :], code)
        wide = jnp.broadcast_to(code, (pair, piece))
        for i, part in enumerate(done):
            cols = slice(i * piece, (i + 1) * piece)
            raw = pool[pl.ds(at, pair), cols].astype(F32)
            pool[pl.ds(at, pair), cols] = jnp.where(wide > 0, part, raw).astype(BF16)

    own_end = tok // block
    cuts = [LAG, LAG + 4, LAG + 8, own_end]
    while cuts[-1] < steps:
        ahead = (cuts[-1] - LAG) // 4 * 4 + 4 + LAG
        cuts.append(min(steps, ahead))

    span = 8 * two

    def combine(at, size, first):
        pick = ones(position[...] == iota((1, size), 1) + at)
        rows = pl.ds(at if isinstance(at, int) else pl.multiple_of(at, two), size)
        for col in range(0, width, piece):
            part = dot(pick, pool[rows, col : col + piece]).astype(BF16)
            if first:
                out_ref[:, col : col + piece] = part
            else:
                out_ref[:, col : col + piece] += part

    whole_at = base + back_blocks * two
    early = REST // 8 - 1

    def step(busy, first, last):
        def run(k, c):
            arrive(k - LAG)

            @pl.when(k >= ring)
            def _():
                sent(k - ring)

            for lo, hi in zip(cuts[:-1], cuts[1:]):
                if hi <= first or lo >= last:
                    continue

                @pl.when((k >= lo) & (k < hi) & (inner | (k < near_blocks)))
                def _():
                    pack(
                        k, tok_at if lo < own_end else base, base + (hi - LAG) * two
                    )

            launch(k)
            if busy:
                m = jnp.where(k < switch, k - HOLD, lax.div(k - LAG - 1, 2))

                @pl.when(
                    ((k < switch) | (lax.rem(k - LAG, 2) == 1)) & (m < mine_pairs + 2)
                )
                def _():
                    work(m)

            return c

        lax.fori_loop(first, last, run, 0)

    switch = 2 * HOLD - LAG
    step(False, LAG, HOLD)

    def gather_local(i, c):
        rank = i * pair + iota((pair, 1), 0)
        at = pl.multiple_of(i * pair, pair)
        pick = ones(rank + LOCAL_KEY == tok_key[...])
        for col in range(0, width, piece):
            pool[pl.ds(at, pair), col : col + piece] = dot(
                pick, pool[tok_at:base, col : col + piece]
            ).astype(BF16)
        return c

    lax.fori_loop(0, 2, gather_local, 0)

    for copy in own:
        copy.wait()
    for copy in arriving:
        copy.wait_recv()
    def heard_dp(i, c):
        total(group, lax.rem(group + i, dps)).wait_recv()
        return c

    lax.fori_loop(1, dps, heard_dp, 0)

    def add_dp(i, carry):
        outer, most = carry
        return (
            outer + total_all[i, 0] * (i < group).astype(jnp.int32),
            jnp.maximum(most, total_all[i, 1]),
        )

    outer, most = lax.fori_loop(0, dps, add_dp, (zero, over))
    offset = before + outer
    flag_ref[...] = most[0:1, 0:1]
    slot = jnp.sum(
        hot_row * offset[:, 0:1].astype(F32), axis=0, keepdims=True
    ).astype(jnp.int32) + rank_row
    slot_ref[...] = slot
    from_row = jnp.where(slot < capacity, from_row, -1)
    position[...] = jnp.transpose(
        jnp.broadcast_to(from_row, (8, tok)).astype(F32)
    )[:, 0:1].astype(jnp.int32)

    step(True, HOLD, steps)
    combine(0, tok_at, True)

    def combine_step(c, carry):
        combine(whole_at + c * span, span, False)
        return carry

    lax.fori_loop(0, early + 2, combine_step, 0)
    rest = whole_at + (early + 2) * span

    def late(b, c):
        take(b)
        return c

    lax.fori_loop(
        jnp.where(inner, steps - LAG, steps - 2 * LAG),
        jnp.where(inner, near_blocks, b_blocks), late, 0,
    )
    combine(rest, pool.shape[0] - rest, False)

    def flush(k, c):
        sent(k)
        return c

    lax.fori_loop(steps - ring, steps, flush, 0)
    for copy in share:
        copy.wait_send()

    def drain(i, c):
        count(lax.rem(me + i, n), me).wait_send()
        return c

    lax.fori_loop(1, n, drain, 0)

    def drain_dp(i, c):
        total(lax.rem(group + i, dps), group).wait_send()
        return c

    lax.fori_loop(1, dps, drain_dp, 0)


def settle_kernel(rows_in, slot_in, rows_out, slot_out):
    rows_out[...] = rows_in[...]
    slot_out[...] = slot_in[...]


def settle_outputs(mixed, slot):
    tok, width = mixed.shape
    parts = 2
    rows = pl.BlockSpec((tok // parts, width), lambda i: (i, 0))
    whole = pl.BlockSpec((1, tok), lambda i: (0, 0))
    mixed, slot = pl.pallas_call(
        settle_kernel,
        grid=(parts,),
        out_shape=(
            jax.ShapeDtypeStruct(mixed.shape, mixed.dtype),
            jax.ShapeDtypeStruct(slot.shape, slot.dtype),
        ),
        in_specs=[rows, whole],
        out_specs=(rows, whole),
    )(mixed, slot)
    return mixed, slot.reshape(tok)


def streamed(tokens, expert_ids, gate_proj, up_proj, down_proj):
    tok, width = tokens.shape
    hidden = gate_proj.shape[2]
    n = lax.axis_size("expert")
    dps = lax.axis_size("dp")
    capacity = tok * dps
    block = tok // (2 * n)
    far_blocks = 9 * n // 2
    near_blocks = far_blocks + 1
    go_blocks = 13 * n // 4
    back_blocks = n
    blocks = near_blocks
    ring = 4
    vmem = pl.BlockSpec(memory_space=pltpu.VMEM)
    anywhere = pl.BlockSpec(memory_space=pltpu.MemorySpace.HBM)
    dma = pltpu.SemaphoreType.DMA
    table = pltpu.VMEM((n, LANES), jnp.int32)
    mixed, slot, flag = pl.pallas_call(
        functools.partial(
            stream_kernel, n, dps, capacity, block, near_blocks, far_blocks, go_blocks,
            back_blocks,
        ),
        out_shape=(
            jax.ShapeDtypeStruct((tok, width), BF16),
            jax.ShapeDtypeStruct((1, tok), jnp.int32),
            jax.ShapeDtypeStruct((1, 1), jnp.int32),
        ),
        in_specs=[vmem, anywhere, anywhere, anywhere, anywhere],
        out_specs=(vmem, vmem, vmem),
        scratch_shapes=[
            pltpu.VMEM((2, width, hidden), BF16),
            pltpu.VMEM((2, width, hidden), BF16),
            pltpu.VMEM((2 * hidden, width), BF16),
            pltpu.VMEM((8 * block + tok + 2 * block * blocks, width), BF16),
            pltpu.VMEM((2 * block * blocks, width), BF16),
            pltpu.VMEM((ring, 2 * block, width), BF16),
            pltpu.VMEM((1, tok), jnp.int32),
            pltpu.VMEM((1, 2 * block * blocks), jnp.int32),
            pltpu.VMEM((tok, 1), jnp.int32),
            table,
            pltpu.VMEM((n, n, LANES), jnp.int32),
            pltpu.VMEM((2, n, LANES), jnp.int32),
            pltpu.VMEM((dps, 2, n, LANES), jnp.int32),
            dma((1,)), dma((3,)), dma((3,)), dma((3,)),
            dma((ring,)), dma((near_blocks,)), dma((ring,)), dma((far_blocks,)),
            dma((n,)), dma((n,)), dma((dps,)), dma((dps,)),
        ],
        compiler_params=pltpu.CompilerParams(
            collective_id=0, has_side_effects=True, vmem_limit_bytes=60 * 2**20
        ),
    )(expert_ids.reshape(1, tok), tokens, gate_proj, up_proj, down_proj)
    return lax.cond(
        flag[0, 0] > 0,
        lambda: padded(tokens, expert_ids, gate_proj, up_proj, down_proj),
        lambda: tuple(settle_outputs(mixed, slot)),
    )


def on_device(tokens, expert_ids, gate_proj, up_proj, down_proj):
    n = lax.axis_size("expert")
    if n == 8 and tokens.shape[0] // n % 64 == 0:
        return streamed(tokens, expert_ids, gate_proj, up_proj, down_proj)
    return direct(tokens, expert_ids, gate_proj, up_proj, down_proj)


def solution(mesh):
    in_specs = (
        P(("dp", "expert"), None),
        P(("dp", "expert"), None),
        P("expert", None, None),
        P("expert", None, None),
        P("expert", None, None),
    )
    out_specs = (P(("dp", "expert"), None), P(("dp", "expert")))
    return jax.shard_map(
        on_device, mesh=mesh, in_specs=in_specs, out_specs=out_specs, check_vma=False
    )
```

```python
import functools

import jax
import jax.numpy as jnp
from jax import lax
from jax.experimental import pallas as pl
from jax.experimental.pallas import tpu as pltpu
from jax.sharding import PartitionSpec as P

MESH = pl.DeviceIdType.MESH
F32 = jnp.float32
BF16 = jnp.bfloat16
LANES = 128
LAG, HOLD, REST = 3, 7, 23


def spread(step, n):
    half = (step // 2) * (2 * (step % 2) - 1)
    return jnp.where(step == 0, 0, n // 2 + half)


def direct_kernel(
    n, dps, most, capacity,
    row_ids, col_ids, tok_ref, gate_hbm, up_hbm, down_hbm,
    out_ref, slot_ref,
    gate_ref, up_ref, down_ref, outgoing, arrived, results, returned,
    position, offset, counts, count_all, totals, total_all,
    weight_sem, go_send, go_recv, back_send, back_recv,
    count_send, count_recv, total_send, total_recv,
):
    me = lax.axis_index("expert")
    group = lax.axis_index("dp")
    tok = tok_ref.shape[0]
    width = tok_ref.shape[1]

    weights = [
        pltpu.make_async_copy(src.at[0], dst, weight_sem.at[i])
        for i, (src, dst) in enumerate(
            ((gate_hbm, gate_ref), (up_hbm, up_ref), (down_hbm, down_ref))
        )
    ]
    for copy in weights:
        copy.start()

    barrier = pltpu.get_barrier_semaphore()

    def greet(i, c):
        pl.semaphore_signal(
            barrier, inc=1, device_id={"expert": lax.rem(me + i, n)}, device_id_type=MESH
        )
        return c

    def greet_dp(i, c):
        pl.semaphore_signal(
            barrier, inc=1, device_id={"dp": lax.rem(group + i, dps)}, device_id_type=MESH
        )
        return c

    lax.fori_loop(1, n, greet, 0)
    lax.fori_loop(1, dps, greet_dp, 0)

    earlier = lax.broadcasted_iota(jnp.int32, (tok, tok), 0) < lax.broadcasted_iota(
        jnp.int32, (tok, tok), 1
    )
    later = lax.broadcasted_iota(jnp.int32, (tok, tok), 0) > lax.broadcasted_iota(
        jnp.int32, (tok, tok), 1
    )
    ids_row = row_ids[...]
    hot_row = (ids_row == lax.broadcasted_iota(jnp.int32, (n, tok), 0)).astype(F32)
    before_row = jnp.dot(
        hot_row.astype(BF16), earlier.astype(F32).astype(BF16), preferred_element_type=F32
    )
    rank_row = jnp.sum(before_row * hot_row, axis=0, keepdims=True).astype(jnp.int32)
    pos_row = ids_row * most + rank_row
    counts[...] = jnp.broadcast_to(
        jnp.sum(hot_row, axis=1, keepdims=True), (n, LANES)
    ).astype(jnp.int32)

    ids_col = col_ids[...]
    hot_col = (ids_col == lax.broadcasted_iota(jnp.int32, (tok, n), 1)).astype(F32)
    before_col = jnp.dot(
        later.astype(F32).astype(BF16), hot_col.astype(BF16), preferred_element_type=F32
    )
    rank_col = jnp.sum(before_col * hot_col, axis=1, keepdims=True).astype(jnp.int32)
    position[...] = ids_col * most + rank_col

    def go(dest, source):
        return pltpu.make_async_remote_copy(
            src_ref=outgoing.at[dest], dst_ref=arrived.at[source],
            send_sem=go_send.at[dest], recv_sem=go_recv.at[source],
            device_id={"expert": dest}, device_id_type=MESH,
        )

    def back(dest, source):
        return pltpu.make_async_remote_copy(
            src_ref=results.at[dest], dst_ref=returned.at[source],
            send_sem=back_send.at[dest], recv_sem=back_recv.at[source],
            device_id={"expert": dest}, device_id_type=MESH,
        )

    def count(dest, source):
        return pltpu.make_async_remote_copy(
            src_ref=counts, dst_ref=count_all.at[source],
            send_sem=count_send.at[dest], recv_sem=count_recv.at[source],
            device_id={"expert": dest}, device_id_type=MESH,
        )

    def total(dest, source):
        return pltpu.make_async_remote_copy(
            src_ref=totals, dst_ref=total_all.at[source],
            send_sem=total_send.at[dest], recv_sem=total_recv.at[source],
            device_id={"dp": dest}, device_id_type=MESH,
        )

    def pack(dest):
        pick = (
            lax.broadcasted_iota(jnp.int32, (most, tok), 0) + dest * most == pos_row
        ).astype(F32).astype(BF16)
        return jnp.dot(pick, tok_ref[...], preferred_element_type=F32).astype(BF16)

    pl.semaphore_wait(barrier, n + dps - 2)

    def dispatch(i, c):
        dest = lax.rem(me + spread(i, n), n)
        outgoing[dest] = pack(dest)
        go(dest, me).start()
        return c

    lax.fori_loop(1, n, dispatch, 0)

    def tell(i, c):
        count(lax.rem(me + i, n), me).start()
        return c

    lax.fori_loop(1, n, tell, 0)
    count_all[me] = counts[...]
    arrived[me] = pack(me)

    for copy in weights:
        copy.wait()

    def ffn(source):
        rows = arrived[source]
        gate = jnp.dot(rows, gate_ref[...], preferred_element_type=F32)
        up = jnp.dot(rows, up_ref[...], preferred_element_type=F32)
        hidden = (gate / (1.0 + jnp.exp(-gate)) * up).astype(BF16)
        return jnp.dot(hidden, down_ref[...], preferred_element_type=F32).astype(BF16)

    def expert_step(i, c):
        source = lax.rem(me + n - spread(i, n), n)

        @pl.when(i > 0)
        def _():
            go(me, source).wait_recv()

        results[source] = ffn(source)

        @pl.when(i > 0)
        def _():
            back(source, me).start()

        return c

    lax.fori_loop(0, n, expert_step, 0)

    def heard(i, c):
        count(me, lax.rem(me + i, n)).wait_recv()
        return c

    lax.fori_loop(1, n, heard, 0)

    def add(i, carry):
        inner, whole = carry
        here = count_all[i]
        return inner + here * (i < me).astype(jnp.int32), whole + here

    zero = jnp.zeros((n, LANES), jnp.int32)
    inner, whole = lax.fori_loop(0, n, add, (zero, zero))
    totals[...] = whole

    def tell_dp(i, c):
        total(lax.rem(group + i, dps), group).start()
        return c

    lax.fori_loop(1, dps, tell_dp, 0)
    total_all[group] = whole

    def heard_dp(i, c):
        total(group, lax.rem(group + i, dps)).wait_recv()
        return c

    lax.fori_loop(1, dps, heard_dp, 0)

    def add_dp(i, outer):
        return outer + total_all[i] * (i < group).astype(jnp.int32)

    offset[...] = inner + lax.fori_loop(0, dps, add_dp, zero)
    slot_ref[...] = (
        jnp.sum(
            hot_row * offset[:, 0:1].astype(F32), axis=0, keepdims=True
        ).astype(jnp.int32)
        + rank_row
    )

    piece = min(width, 512)

    def combine(source, block, first):
        lane = lax.broadcasted_iota(jnp.int32, (tok, most), 1)
        fits = offset[pl.ds(source, 1), 0:most] + lax.broadcasted_iota(
            jnp.int32, (1, most), 1
        ) < capacity
        pick = (lane + source * most == position[...]) & fits
        pick = pick.astype(F32).astype(BF16)
        for at in range(0, width, piece):
            part = jnp.dot(
                pick, block[source, :, at : at + piece], preferred_element_type=F32
            ).astype(BF16)
            if first:
                out_ref[:, at : at + piece] = part
            else:
                out_ref[:, at : at + piece] += part

    combine(me, results, True)

    def combine_step(i, c):
        source = lax.rem(me + n - spread(i, n), n)
        back(me, source).wait_recv()
        combine(source, returned, False)
        return c

    lax.fori_loop(1, n, combine_step, 0)

    def drain(i, c):
        other = lax.rem(me + i, n)
        go(other, me).wait_send()
        back(other, me).wait_send()
        count(other, me).wait_send()
        return c

    lax.fori_loop(1, n, drain, 0)

    def drain_dp(i, c):
        total(lax.rem(group + i, dps), group).wait_send()
        return c

    lax.fori_loop(1, dps, drain_dp, 0)


def direct(tokens, expert_ids, gate_proj, up_proj, down_proj):
    tok, width = tokens.shape
    hidden = gate_proj.shape[2]
    n = lax.axis_size("expert")
    dps = lax.axis_size("dp")
    most = 2 * tok // n
    capacity = tok * dps
    vmem = pl.BlockSpec(memory_space=pltpu.VMEM)
    anywhere = pl.BlockSpec(memory_space=pltpu.MemorySpace.HBM)
    dma = pltpu.SemaphoreType.DMA
    block = pltpu.VMEM((n, most, width), BF16)
    mixed, slot = pl.pallas_call(
        functools.partial(direct_kernel, n, dps, most, capacity),
        out_shape=(
            jax.ShapeDtypeStruct((tok, width), BF16),
            jax.ShapeDtypeStruct((1, tok), jnp.int32),
        ),
        in_specs=[vmem, vmem, vmem, anywhere, anywhere, anywhere],
        out_specs=(vmem, vmem),
        scratch_shapes=[
            pltpu.VMEM((width, hidden), BF16),
            pltpu.VMEM((width, hidden), BF16),
            pltpu.VMEM((hidden, width), BF16),
            block, block, block, block,
            pltpu.VMEM((tok, 1), jnp.int32),
            pltpu.VMEM((n, LANES), jnp.int32),
            pltpu.VMEM((n, LANES), jnp.int32),
            pltpu.VMEM((n, n, LANES), jnp.int32),
            pltpu.VMEM((n, LANES), jnp.int32),
            pltpu.VMEM((dps, n, LANES), jnp.int32),
            dma((3,)), dma((n,)), dma((n,)), dma((n,)), dma((n,)),
            dma((n,)), dma((n,)), dma((dps,)), dma((dps,)),
        ],
        compiler_params=pltpu.CompilerParams(
            collective_id=0, has_side_effects=True, vmem_limit_bytes=60 * 2**20
        ),
    )(
        expert_ids.reshape(1, tok), expert_ids, tokens, gate_proj, up_proj, down_proj
    )
    return mixed, slot.reshape(tok)


def entering(part, axis, combine, identity):
    place = lax.axis_index(axis)
    gathered = lax.all_gather(part, axis)
    state = jnp.zeros_like(part) + jnp.asarray(identity, part.dtype)

    def one(hop, state):
        return combine(state, lax.dynamic_index_in_dim(gathered, hop, 0, False))

    return lax.fori_loop(0, place, one, state)


def add_counts(earlier, later):
    return earlier + later


def expert_ffn(rows, gate_proj, up_proj, down_proj):
    gate_val = jnp.dot(rows, gate_proj[0], preferred_element_type=jnp.float32)
    up_val = jnp.dot(rows, up_proj[0], preferred_element_type=jnp.float32)
    hidden = (jax.nn.silu(gate_val) * up_val).astype(jnp.bfloat16)
    return jnp.dot(hidden, down_proj[0], preferred_element_type=jnp.float32).astype(jnp.bfloat16)


def padded(tokens, expert_ids, gate_proj, up_proj, down_proj):
    tok_rows, width = tokens.shape
    experts_all = lax.axis_size("expert")
    most = 2 * tok_rows // experts_all
    capacity = tok_rows * lax.axis_size("dp")
    choices = expert_ids[:, 0]
    onehot = (choices[:, None] == jnp.arange(experts_all, dtype=jnp.int32)[None, :]).astype(
        jnp.int32
    )
    counts = jnp.sum(onehot, axis=0)
    inner = entering(counts, "expert", add_counts, jnp.zeros_like(counts))
    totals = lax.psum(counts, "expert")
    outer = entering(totals, "dp", add_counts, jnp.zeros_like(totals))
    offset = inner + outer
    before = jnp.cumsum(onehot, axis=0) - onehot
    local_rank = jnp.sum(before * onehot, axis=1)
    global_slot = (jnp.sum(onehot * offset[None, :], axis=1) + local_rank).astype(jnp.int32)
    is_kept = global_slot < capacity
    position = choices * most + local_rank
    targets = jnp.arange(experts_all * most, dtype=jnp.int32)
    dispatch = ((targets[:, None] == position[None, :]) & is_kept[None, :]).astype(jnp.bfloat16)
    outgoing = jnp.dot(dispatch, tokens, preferred_element_type=jnp.float32).astype(jnp.bfloat16)
    outgoing = outgoing.reshape(experts_all, most, width)
    arrived = lax.all_to_all(outgoing, "expert", split_axis=0, concat_axis=0, tiled=True)
    sources, slots_here, _ = arrived.shape
    flat = arrived.reshape(sources * slots_here, width)
    returned = lax.all_to_all(
        expert_ffn(flat, gate_proj, up_proj, down_proj).reshape(sources, slots_here, width),
        "expert",
        split_axis=0,
        concat_axis=0,
        tiled=True,
    )
    flat_back = returned.reshape(experts_all * most, width)
    mixed = lax.dot_general(
        dispatch, flat_back, (((0,), (0,)), ((), ())), preferred_element_type=jnp.float32
    )
    return (mixed.astype(jnp.bfloat16), global_slot)


RUN_ORDER = {
    "A": ("go oq", "go op", "go oi", "ret op", "ret oq", "ret oi"),
    "M": (
        "go ip", "go iq", "go oq", "go op", "ret ip", "ret op", "ret iq", "ret oq",
    ),
    "B": ("go io", "go po", "go qo", "ret io", "ret po", "ret qo"),
}
FLIP = {"o": "q", "i": "p", "p": "i", "q": "o"}
FAR_KEY = 4096
LOCAL_KEY = 8192


def lay_streams(rows_of, block):
    place, end = {}, {}
    queue = {
        (s, h): [(run[:-3], run[-2], run[-1]) for run in RUN_ORDER[s]]
        for s in "AMB" for h in (0, 1)
    }
    zero = jnp.zeros((1, LANES), jnp.int32)
    for name in queue:
        end[name] = zero
    while any(queue.values()):
        for (s, h), runs in queue.items():
            while runs:
                kind, a, b = runs[0]
                fa, fb = FLIP[a], FLIP[b]
                need, result = None, kind == "ret"
                if s == "A" and kind == "ret":
                    need = ("B", h, "go", b, a)
                elif s == "M" and a == "o":
                    need, result = ("A", h, kind, a, b), False
                elif s == "M" and kind == "ret":
                    need = ("M", 1 - h, "go", fb, fa)
                elif s == "B" and a != "i":
                    need, result = ("M", 1 - h, kind, fa, fb), False
                elif s == "B" and kind == "ret":
                    need = ("A", h, "go", b, a)
                if need is not None and need not in place:
                    break
                size = rows_of(h, a, b) if kind == "go" else rows_of(h, b, a)
                first = end[(s, h)]
                if need is not None:
                    there = place[need][0]
                    ready = there + block * LAG
                    if result:
                        ready = jnp.maximum(
                            ready + block * 2,
                            lax.shift_right_logical(there, 1) + block * (HOLD + 1),
                        )
                    if s == "B":
                        ready -= block * jnp.clip(ready // block - REST, 0, LAG)
                    first = jnp.where(size > 0, jnp.maximum(first, ready), first)
                place[(s, h, kind, a, b)] = (first, size)
                end[(s, h)] = first + size
                runs.pop(0)
    return place, end


def stream_kernel(
    n, dps, capacity, block, near_blocks, far_blocks, go_blocks, back_blocks,
    row_ids, tok_hbm, gate_hbm, up_hbm, down_hbm,
    out_ref, slot_ref, flag_ref,
    gate_ref, up_ref, down_ref, pool, inbox, outbox,
    tok_key, in_key, position, counts, count_all, totals, total_all,
    tok_sem, own_sem, pair_send, pair_recv, near_send, near_recv, far_send, far_recv,
    count_send, count_recv, total_send, total_recv,
):
    me = lax.axis_index("expert")
    group = lax.axis_index("dp")
    tok = row_ids.shape[1]
    width = pool.shape[1]
    hidden = gate_ref.shape[2]
    core = lax.rem(me, 2)
    chip = lax.div(me, 2)
    half = lax.div(chip, 2)
    roles = {"o": 3 * half, "i": 1 + half, "p": 2 - half, "q": 3 - 3 * half}
    inner = chip == roles["i"]
    is_inner = inner.astype(jnp.int32)
    near_dev = me + 2 - 4 * lax.rem(chip, 2)
    far_dev = 2 * (3 - chip) + core
    pair_dev = me + 1 - 2 * core
    two = 2 * block
    blocks = inbox.shape[0] // two
    pair = 2 * two
    steps = far_blocks + LAG
    b_blocks = far_blocks
    tok_at = 2 * pair
    base = tok_at + tok
    piece = min(width, 1024)
    ring = outbox.shape[0]

    def iota(shape, axis):
        return lax.broadcasted_iota(jnp.int32, shape, axis)

    def ones(mask):
        return mask.astype(F32).astype(BF16)

    def dot(a, b):
        return jnp.dot(a, b, preferred_element_type=F32)

    load_tok = pltpu.make_async_copy(tok_hbm, pool.at[pl.ds(tok_at, tok)], tok_sem.at[0])
    load_tok.start()
    mine_down = pl.ds(pl.multiple_of(core * hidden, hidden), hidden)
    pairs = (
        (gate_hbm, gate_ref.at[core]), (up_hbm, up_ref.at[core]),
        (down_hbm, down_ref.at[mine_down]),
    )
    own = [
        pltpu.make_async_copy(src.at[0], dst, own_sem.at[i])
        for i, (src, dst) in enumerate(pairs)
    ]
    share = [
        pltpu.make_async_remote_copy(
            src_ref=src.at[0], dst_ref=dst, send_sem=pair_send.at[i],
            recv_sem=pair_recv.at[i], device_id={"expert": pair_dev}, device_id_type=MESH,
        )
        for i, (src, dst) in enumerate(pairs)
    ]
    other_down = pl.ds(pl.multiple_of((1 - core) * hidden, hidden), hidden)
    arriving = [
        pltpu.make_async_remote_copy(
            src_ref=src.at[0], dst_ref=dst, send_sem=pair_send.at[i],
            recv_sem=pair_recv.at[i], device_id={"expert": pair_dev}, device_id_type=MESH,
        )
        for i, (src, dst) in enumerate((
            (gate_hbm, gate_ref.at[1 - core]), (up_hbm, up_ref.at[1 - core]),
            (down_hbm, down_ref.at[other_down]),
        ))
    ]
    for copy in own:
        copy.start()

    barrier = pltpu.get_barrier_semaphore()

    def greet(i, c):
        pl.semaphore_signal(
            barrier, inc=1, device_id={"expert": lax.rem(me + i, n)}, device_id_type=MESH
        )
        return c

    def greet_dp(i, c):
        pl.semaphore_signal(
            barrier, inc=1, device_id={"dp": lax.rem(group + i, dps)}, device_id_type=MESH
        )
        return c

    lax.fori_loop(1, n, greet, 0)
    lax.fori_loop(1, dps, greet_dp, 0)

    ids_row = row_ids[...]
    hot_row = (ids_row == iota((n, tok), 0)).astype(F32)
    earlier = ones(iota((LANES, LANES), 0) < iota((LANES, LANES), 1))
    ahead, mine = [], jnp.zeros((n, 1), F32)
    for lo in range(0, tok, LANES):
        hot = hot_row[:, lo : lo + LANES]
        ahead.append(dot(hot.astype(BF16), earlier) + mine)
        mine = mine + jnp.sum(hot, axis=1, keepdims=True)
    before_row = jnp.concatenate(ahead, axis=1)
    rank_row = jnp.sum(before_row * hot_row, axis=0, keepdims=True).astype(jnp.int32)
    mine = jnp.broadcast_to(mine, (n, LANES))
    counts[...] = mine.astype(jnp.int32)
    row8 = iota((n, n), 0)
    shift = ones((iota((n, n), 1) + 1 == row8) & (lax.rem(row8, 2) == 1))
    skip = dot(shift, mine.astype(BF16))
    pair_rank = rank_row + jnp.sum(
        hot_row * skip[:, 0:1], axis=0, keepdims=True
    ).astype(jnp.int32)
    pair_row = lax.shift_right_logical(ids_row, 1)

    def own_rows(role):
        e = 2 * roles[role]
        return (counts[pl.ds(e, 1), :] + counts[pl.ds(e + 1, 1), :])[:, 0:1]

    zero1 = jnp.zeros((1, 1), jnp.int32)
    to_o = jnp.where(inner, zero1, LOCAL_KEY)
    to_i = jnp.where(inner, LOCAL_KEY, own_rows("p") + own_rows("q"))
    to_p = jnp.where(inner, FAR_KEY, own_rows("q"))
    to_q = jnp.where(inner, FAR_KEY + own_rows("p"), 0)
    key = jnp.zeros((1, tok), jnp.int32)
    for role, to in (("o", to_o), ("i", to_i), ("p", to_p), ("q", to_q)):
        key = jnp.where(pair_row == roles[role], to + pair_rank, key)
    tok_key[...] = key

    def near_copy(j, slot):
        return pltpu.make_async_remote_copy(
            src_ref=outbox.at[slot, pl.ds(0, block)],
            dst_ref=inbox.at[pl.ds(pl.multiple_of(j * two, two), block)],
            send_sem=near_send.at[slot], recv_sem=near_recv.at[j],
            device_id={"expert": near_dev}, device_id_type=MESH,
        )

    def far_copy(j, slot):
        return pltpu.make_async_remote_copy(
            src_ref=outbox.at[slot, pl.ds(block, block)],
            dst_ref=inbox.at[pl.ds(pl.multiple_of(j * two + block, block), block)],
            send_sem=far_send.at[slot], recv_sem=far_recv.at[j],
            device_id={"expert": far_dev}, device_id_type=MESH,
        )

    def count(dest, source):
        return pltpu.make_async_remote_copy(
            src_ref=counts, dst_ref=count_all.at[source],
            send_sem=count_send.at[dest], recv_sem=count_recv.at[source],
            device_id={"expert": dest}, device_id_type=MESH,
        )

    def total(dest, source):
        return pltpu.make_async_remote_copy(
            src_ref=totals, dst_ref=total_all.at[source],
            send_sem=total_send.at[dest], recv_sem=total_recv.at[source],
            device_id={"dp": dest}, device_id_type=MESH,
        )

    def near_at(k, rests):
        return k - rests * jnp.where(k < REST + LAG, 0, LAG)

    def near_on(k, rests):
        idle = rests * jnp.where((k >= REST) & (k < REST + LAG), 1, 0)
        return (idle == 0) & (k < near_blocks + rests * (steps - near_blocks))

    def far_on(k):
        return inner & (k < far_blocks)

    def sent(k):
        slot = lax.rem(k, ring)

        @pl.when(near_on(k, is_inner))
        def _():
            near_copy(near_at(k, is_inner), slot).wait_send()

        @pl.when(far_on(k))
        def _():
            far_copy(k, slot).wait_send()

    def pack(k, low, high):
        slot = lax.rem(k, ring)
        row = iota((two, 1), 0)
        want = jnp.where(
            row < block, near_at(k, is_inner) * block + row, FAR_KEY + k * block + row - block
        )
        picks = []
        if low < base:
            picks.append(ones(want == tok_key[...]))
        if high > base:
            picks.append(ones(want == in_key[:, max(low, base) - base : high - base]))
        pick = picks[0] if len(picks) == 1 else jnp.concatenate(picks, axis=1)
        for at in range(0, width, piece):
            outbox[slot, :, at : at + piece] = dot(
                pick, pool[low:high, at : at + piece]
            ).astype(BF16)

    def launch(k):
        slot = lax.rem(k, ring)

        @pl.when(near_on(k, is_inner))
        def _():
            near_copy(near_at(k, is_inner), slot).start()

        @pl.when(far_on(k))
        def _():
            far_copy(k, slot).start()

    def take(b):
        at = pl.multiple_of(b * two, two)
        near_copy(b, 0).wait_recv()
        pool[pl.ds(base + at, block), :] = inbox[pl.ds(at, block), :]

    def arrive(k):
        @pl.when(near_on(k, 1 - is_inner))
        def _():
            take(near_at(k, 1 - is_inner))

        @pl.when(far_on(k))
        def _():
            far_copy(k, 0).wait_recv()
            at = pl.multiple_of(k * two, two)
            pool[pl.ds(base + at + block, block), :] = inbox[pl.ds(at + block, block), :]

    def ffn(rows, code):
        parts = []
        wide = jnp.broadcast_to(code, (pair, hidden))
        for parity in (0, 1):
            gate = dot(rows, gate_ref[parity])
            up = dot(rows, up_ref[parity])
            act = gate / (1.0 + jnp.exp(-gate)) * up
            parts.append(jnp.where(wide == parity + 1, act, 0.0).astype(BF16))
        act = jnp.concatenate(parts, axis=1)
        return [
            dot(act, down_ref[:, at : at + piece]) for at in range(0, width, piece)
        ]

    load_tok.wait()
    pack(0, tok_at, base)
    pl.semaphore_wait(barrier, n + dps - 2)
    launch(0)

    def tell(i, c):
        count(lax.rem(me + i, n), me).start()
        return c

    lax.fori_loop(1, n, tell, 0)
    for copy in share:
        copy.start()
    for k in range(1, LAG):
        pack(k, tok_at, base)
        launch(k)
    count_all[me] = counts[...]

    spare = pool.at[pl.ds(base, blocks * two)]

    def clear(i, c):
        spare[pl.ds(pl.multiple_of(i * two, two), two), :] = jnp.zeros((two, width), BF16)
        return c

    lax.fori_loop(0, blocks, clear, 0)

    def heard(i, c):
        count(me, lax.rem(me + i, n)).wait_recv()
        return c

    lax.fori_loop(1, n, heard, 0)

    def rows_of(lane):
        def get(h, a, b):
            a, b = (FLIP[a], FLIP[b]) if h else (a, b)
            dev, e = 2 * roles[a] + lane, 2 * roles[b]
            return count_all[dev, pl.ds(e, 1), :] + count_all[dev, pl.ds(e + 1, 1), :]

        return get

    def even(a):
        return count_all[2 * roles[a] + core, pl.ds(2 * chip, 1), :][:, 0:1]

    place, ends = lay_streams(rows_of(core), block)
    over = jnp.zeros((1, LANES), jnp.int32)
    for lane_place, lane_ends in (
        (place, ends), lay_streams(rows_of(1 - core), block)
    ):
        for (s, _), end in lane_ends.items():
            limit = {"A": near_blocks, "M": far_blocks, "B": b_blocks}[s] * block
            over = jnp.maximum(over, (end > limit).astype(jnp.int32))
        for name, (first, size) in lane_place.items():
            if name[2] == "go":
                limit = (REST if name[0] == "B" else go_blocks) * block
                bad = (first + size > limit) & (size > 0)
            else:
                bad = (first < back_blocks * block) & (size > 0)
            over = jnp.maximum(over, bad.astype(jnp.int32))

    def at(name):
        first, size = place[name]
        return first[:, 0:1], size[:, 0:1]

    def choose(a, b):
        return tuple(jnp.where(inner, x, y) for x, y in zip(at(a), at(b)))

    def start(name):
        return at(name)[0]

    lane = iota((1, blocks * two), 1)
    inside = lax.rem(lane, two)
    is_far = inside >= block
    spot = lax.div(lane, two) * block + lax.rem(inside, block)
    nowhere = zero1 - 65536
    code = jnp.full((1, blocks * two), -1, jnp.int32)
    near_runs = (
        (("A", 0, "go", "o", "p"), ("B", 0, "go", "i", "o"),
         FAR_KEY + start(("M", 0, "go", "o", "p")), start(("A", 0, "ret", "o", "i"))),
        (("A", 0, "go", "o", "q"), ("B", 0, "go", "p", "o"),
         FAR_KEY + start(("M", 0, "go", "o", "q")), start(("A", 0, "ret", "o", "p"))),
        (("A", 0, "go", "o", "i"), ("B", 0, "go", "q", "o"),
         start(("B", 0, "ret", "i", "o")), start(("A", 0, "ret", "o", "q"))),
        (("A", 0, "ret", "o", "p"), ("B", 0, "ret", "p", "o"),
         FAR_KEY + start(("M", 0, "ret", "o", "p")), nowhere),
        (("A", 0, "ret", "o", "q"), ("B", 0, "ret", "q", "o"),
         FAR_KEY + start(("M", 0, "ret", "o", "q")), nowhere),
    )
    for in_run, out_run, to_in, to_out in near_runs:
        first, size = choose(in_run, out_run)
        to = jnp.where(inner, to_in, to_out)
        hit = (spot >= first) & (spot < first + size) & jnp.logical_not(is_far)
        code = jnp.where(hit, spot + (to - first), code)
    far_runs = (
        (("M", 1, "go", "i", "p"), FAR_KEY + start(("M", 0, "ret", "i", "p"))),
        (("M", 1, "go", "i", "q"), start(("B", 0, "go", "p", "o"))),
        (("M", 1, "go", "o", "p"), FAR_KEY + start(("M", 0, "ret", "i", "q"))),
        (("M", 1, "go", "o", "q"), start(("B", 0, "go", "q", "o"))),
        (("M", 1, "ret", "i", "q"), start(("B", 0, "ret", "p", "o"))),
        (("M", 1, "ret", "o", "q"), start(("B", 0, "ret", "q", "o"))),
    )
    for run, to in far_runs:
        first, size = at(run)
        hit = (spot >= first) & (spot < first + size) & is_far
        code = jnp.where(hit, spot + (to - first), code)
    in_key[...] = code

    mine_runs = []
    for in_run, out_run, far_side, a_in, a_out in (
        (("A", 0, "go", "o", "i"), ("B", 0, "go", "i", "o"), 0, "o", "i"),
        (("M", 1, "go", "i", "p"), ("B", 0, "go", "p", "o"), 1, "p", "p"),
        (("M", 1, "go", "o", "p"), ("B", 0, "go", "q", "o"), 1, "q", "q"),
    ):
        first, size = choose(in_run, out_run)
        split = jnp.where(inner, even(a_in), even(a_out))
        mine_runs.append((first, size, split, far_side * is_inner))

    mine_pairs = go_blocks // 2

    def mark(m):
        row = iota((pair, 1), 0)
        side = lax.div(lax.rem(row, two), block)
        spot = (2 * m + lax.div(row, two)) * block + lax.rem(row, block)
        code = jnp.zeros((pair, 1), jnp.int32)
        for first, size, split, which in mine_runs:
            hit = (spot >= first) & (spot < first + size) & (side == which)
            code = jnp.where(hit, jnp.where(spot - first >= split, 2, 1), code)
        rank = (m - mine_pairs) * pair + row
        first = counts[pl.ds(2 * chip, 1), :][:, 0:1]
        both = first + counts[pl.ds(2 * chip + 1, 1), :][:, 0:1]
        local = jnp.where(rank < both, jnp.where(rank >= first, 2, 1), 0)
        return jnp.where(m < mine_pairs, code, local)

    home = zero1

    def pool_at(run, side):
        def get(rank):
            spot = start(run) + rank
            return (
                base + lax.div(spot, block) * two + lax.rem(spot, block) + side * block
            )

        return get

    back_in = {
        "o": pool_at(("A", 0, "ret", "o", "i"), 0),
        "p": pool_at(("M", 1, "ret", "i", "p"), 1),
        "q": pool_at(("M", 1, "ret", "o", "p"), 1),
        "i": lambda rank: home + rank,
    }
    back_out = {
        "i": pool_at(("B", 0, "ret", "i", "o"), 0),
        "p": pool_at(("B", 0, "ret", "p", "o"), 0),
        "q": pool_at(("B", 0, "ret", "q", "o"), 0),
        "o": lambda rank: home + rank,
    }
    from_row = jnp.zeros((1, tok), jnp.int32)
    for role in "oipq":
        found = jnp.where(inner, back_in[role](pair_rank), back_out[role](pair_rank))
        from_row = jnp.where(pair_row == roles[role], found, from_row)

    def add(i, carry):
        before, whole = carry
        here = count_all[i]
        return before + here * (i < me).astype(jnp.int32), whole + here

    zero = jnp.zeros((n, LANES), jnp.int32)
    before, whole = lax.fori_loop(0, n, add, (zero, zero))
    over = jnp.broadcast_to(over, (n, LANES))
    totals[0] = whole
    totals[1] = over
    total_all[group, 0] = whole
    total_all[group, 1] = over

    def tell_dp(i, c):
        total(lax.rem(group + i, dps), group).start()
        return c

    lax.fori_loop(1, dps, tell_dp, 0)

    def work(m):
        at = jnp.where(m < mine_pairs, base + m * pair, (m - mine_pairs) * pair)
        at = pl.multiple_of(at, pair)
        code = mark(m)
        done = ffn(pool[pl.ds(at, pair), :], code)
        wide = jnp.broadcast_to(code, (pair, piece))
        for i, part in enumerate(done):
            cols = slice(i * piece, (i + 1) * piece)
            raw = pool[pl.ds(at, pair), cols].astype(F32)
            pool[pl.ds(at, pair), cols] = jnp.where(wide > 0, part, raw).astype(BF16)

    own_end = tok // block
    cuts = [LAG, LAG + 4, LAG + 8, own_end]
    while cuts[-1] < steps:
        ahead = (cuts[-1] - LAG) // 4 * 4 + 4 + LAG
        cuts.append(min(steps, ahead))

    span = 8 * two

    def combine(at, size, first):
        pick = ones(position[...] == iota((1, size), 1) + at)
        rows = pl.ds(at if isinstance(at, int) else pl.multiple_of(at, two), size)
        for col in range(0, width, piece):
            part = dot(pick, pool[rows, col : col + piece]).astype(BF16)
            if first:
                out_ref[:, col : col + piece] = part
            else:
                out_ref[:, col : col + piece] += part

    whole_at = base + back_blocks * two
    early = REST // 8 - 1

    def step(busy, first, last):
        def run(k, c):
            arrive(k - LAG)

            @pl.when(k >= ring)
            def _():
                sent(k - ring)

            for lo, hi in zip(cuts[:-1], cuts[1:]):
                if hi <= first or lo >= last:
                    continue

                @pl.when((k >= lo) & (k < hi) & (inner | (k < near_blocks)))
                def _():
                    pack(
                        k, tok_at if lo < own_end else base, base + (hi - LAG) * two
                    )

            launch(k)
            if busy:
                m = jnp.where(k < switch, k - HOLD, lax.div(k - LAG - 1, 2))

                @pl.when(
                    ((k < switch) | (lax.rem(k - LAG, 2) == 1)) & (m < mine_pairs + 2)
                )
                def _():
                    work(m)

            return c

        lax.fori_loop(first, last, run, 0)

    switch = 2 * HOLD - LAG
    step(False, LAG, HOLD)

    def gather_local(i, c):
        rank = i * pair + iota((pair, 1), 0)
        at = pl.multiple_of(i * pair, pair)
        pick = ones(rank + LOCAL_KEY == tok_key[...])
        for col in range(0, width, piece):
            pool[pl.ds(at, pair), col : col + piece] = dot(
                pick, pool[tok_at:base, col : col + piece]
            ).astype(BF16)
        return c

    lax.fori_loop(0, 2, gather_local, 0)

    for copy in own:
        copy.wait()
    for copy in arriving:
        copy.wait_recv()
    def heard_dp(i, c):
        total(group, lax.rem(group + i, dps)).wait_recv()
        return c

    lax.fori_loop(1, dps, heard_dp, 0)

    def add_dp(i, carry):
        outer, most = carry
        return (
            outer + total_all[i, 0] * (i < group).astype(jnp.int32),
            jnp.maximum(most, total_all[i, 1]),
        )

    outer, most = lax.fori_loop(0, dps, add_dp, (zero, over))
    offset = before + outer
    flag_ref[...] = most[0:1, 0:1]
    slot = jnp.sum(
        hot_row * offset[:, 0:1].astype(F32), axis=0, keepdims=True
    ).astype(jnp.int32) + rank_row
    slot_ref[...] = slot
    from_row = jnp.where(slot < capacity, from_row, -1)
    position[...] = jnp.transpose(
        jnp.broadcast_to(from_row, (8, tok)).astype(F32)
    )[:, 0:1].astype(jnp.int32)

    step(True, HOLD, steps)
    combine(0, tok_at, True)

    def combine_step(c, carry):
        combine(whole_at + c * span, span, False)
        return carry

    lax.fori_loop(0, early + 2, combine_step, 0)
    rest = whole_at + (early + 2) * span

    def late(b, c):
        take(b)
        return c

    lax.fori_loop(
        jnp.where(inner, steps - LAG, steps - 2 * LAG),
        jnp.where(inner, near_blocks, b_blocks), late, 0,
    )
    combine(rest, pool.shape[0] - rest, False)

    def flush(k, c):
        sent(k)
        return c

    lax.fori_loop(steps - ring, steps, flush, 0)
    for copy in share:
        copy.wait_send()

    def drain(i, c):
        count(lax.rem(me + i, n), me).wait_send()
        return c

    lax.fori_loop(1, n, drain, 0)

    def drain_dp(i, c):
        total(lax.rem(group + i, dps), group).wait_send()
        return c

    lax.fori_loop(1, dps, drain_dp, 0)


def settle_kernel(rows_in, slot_in, rows_out, slot_out):
    rows_out[...] = rows_in[...]
    slot_out[...] = slot_in[...]


def settle_outputs(mixed, slot):
    tok, width = mixed.shape
    parts = 2
    rows = pl.BlockSpec((tok // parts, width), lambda i: (i, 0))
    whole = pl.BlockSpec((1, tok), lambda i: (0, 0))
    mixed, slot = pl.pallas_call(
        settle_kernel,
        grid=(parts,),
        out_shape=(
            jax.ShapeDtypeStruct(mixed.shape, mixed.dtype),
            jax.ShapeDtypeStruct(slot.shape, slot.dtype),
        ),
        in_specs=[rows, whole],
        out_specs=(rows, whole),
    )(mixed, slot)
    return mixed, slot.reshape(tok)


def streamed(tokens, expert_ids, gate_proj, up_proj, down_proj):
    tok, width = tokens.shape
    hidden = gate_proj.shape[2]
    n = lax.axis_size("expert")
    dps = lax.axis_size("dp")
    capacity = tok * dps
    block = tok // (2 * n)
    far_blocks = 9 * n // 2
    near_blocks = far_blocks
    go_blocks = 13 * n // 4
    back_blocks = n
    blocks = near_blocks
    ring = 4
    vmem = pl.BlockSpec(memory_space=pltpu.VMEM)
    anywhere = pl.BlockSpec(memory_space=pltpu.MemorySpace.HBM)
    dma = pltpu.SemaphoreType.DMA
    table = pltpu.VMEM((n, LANES), jnp.int32)
    mixed, slot, flag = pl.pallas_call(
        functools.partial(
            stream_kernel, n, dps, capacity, block, near_blocks, far_blocks, go_blocks,
            back_blocks,
        ),
        out_shape=(
            jax.ShapeDtypeStruct((tok, width), BF16),
            jax.ShapeDtypeStruct((1, tok), jnp.int32),
            jax.ShapeDtypeStruct((1, 1), jnp.int32),
        ),
        in_specs=[vmem, anywhere, anywhere, anywhere, anywhere],
        out_specs=(vmem, vmem, vmem),
        scratch_shapes=[
            pltpu.VMEM((2, width, hidden), BF16),
            pltpu.VMEM((2, width, hidden), BF16),
            pltpu.VMEM((2 * hidden, width), BF16),
            pltpu.VMEM((8 * block + tok + 2 * block * blocks, width), BF16),
            pltpu.VMEM((2 * block * blocks, width), BF16),
            pltpu.VMEM((ring, 2 * block, width), BF16),
            pltpu.VMEM((1, tok), jnp.int32),
            pltpu.VMEM((1, 2 * block * blocks), jnp.int32),
            pltpu.VMEM((tok, 1), jnp.int32),
            table,
            pltpu.VMEM((n, n, LANES), jnp.int32),
            pltpu.VMEM((2, n, LANES), jnp.int32),
            pltpu.VMEM((dps, 2, n, LANES), jnp.int32),
            dma((1,)), dma((3,)), dma((3,)), dma((3,)),
            dma((ring,)), dma((near_blocks,)), dma((ring,)), dma((far_blocks,)),
            dma((n,)), dma((n,)), dma((dps,)), dma((dps,)),
        ],
        compiler_params=pltpu.CompilerParams(
            collective_id=0, has_side_effects=True, vmem_limit_bytes=60 * 2**20
        ),
    )(expert_ids.reshape(1, tok), tokens, gate_proj, up_proj, down_proj)
    return lax.cond(
        flag[0, 0] > 0,
        lambda: padded(tokens, expert_ids, gate_proj, up_proj, down_proj),
        lambda: tuple(settle_outputs(mixed, slot)),
    )


def on_device(tokens, expert_ids, gate_proj, up_proj, down_proj):
    n = lax.axis_size("expert")
    if n == 8 and tokens.shape[0] // n % 64 == 0:
        return streamed(tokens, expert_ids, gate_proj, up_proj, down_proj)
    return direct(tokens, expert_ids, gate_proj, up_proj, down_proj)


def solution(mesh):
    in_specs = (
        P(("dp", "expert"), None),
        P(("dp", "expert"), None),
        P("expert", None, None),
        P("expert", None, None),
        P("expert", None, None),
    )
    out_specs = (P(("dp", "expert"), None), P(("dp", "expert")))
    return jax.shard_map(
        on_device, mesh=mesh, in_specs=in_specs, out_specs=out_specs, check_vma=False
    )
```
